32 devices in a mesh: pipe: 4 (over z), expert: 4 (over y, x), tensor: 2 (over core).
Axes of the slice: x: 2, y: 2, z: 4, core: 2. Of those that a mesh axis runs over, the one named last changes fastest.
Arguments:
- inputs_prev: bfloat16 [4, 512, 3584], P('pipe', 'expert', 'tensor'), may hold values from -6 to 6
- cotangent_next: bfloat16 [4, 512, 3584], P('pipe', 'expert', 'tensor'), may hold values from -6 to 6
- saved_input: bfloat16 [4, 512, 3584], P('pipe', 'expert', 'tensor'), may hold values from -6 to 6
- expert_ids: int32 [2, 4, 512, 8], P(None, 'pipe', 'expert'), may hold values from 0 to 255, as said below
- keep_mask: int32 [2, 4, 512, 8], P(None, 'pipe', 'expert'), may hold values from 0 to 1, as said below
- slot_pos: int32 [2, 4, 512, 8], P(None, 'pipe', 'expert'), may hold values from 0 to 3, as said below
- weight_q: int32 [2, 4, 512, 8], P(None, 'pipe', 'expert'), may hold values from 1 to 4095
- gate_routed: bfloat16 [4, 4, 3584, 512], P('pipe', 'expert', None, 'tensor'), may hold values from -0.09375 to 0.09375
- up_routed: bfloat16 [4, 4, 3584, 512], P('pipe', 'expert', None, 'tensor'), may hold values from -0.09375 to 0.09375
- down_routed: bfloat16 [4, 4, 512, 3584], P('pipe', 'expert', 'tensor'), may hold values from -0.1875 to 0.1875
- gate_shared: bfloat16 [4, 3584, 1024], P('pipe', None, 'tensor'), may hold values from -0.09375 to 0.09375
- up_shared: bfloat16 [4, 3584, 1024], P('pipe', None, 'tensor'), may hold values from -0.09375 to 0.09375
- down_shared: bfloat16 [4, 1024, 3584], P('pipe', 'tensor'), may hold values from -0.1875 to 0.1875
Outputs:
- out_act: bfloat16 [4, 512, 3584], P('pipe', 'expert', 'tensor')
- in_grad: bfloat16 [4, 512, 3584], P('pipe', 'expert', 'tensor')
The draws below stay inside these ranges and needn't reach their ends.
Inputs may be any that keep to these rules, and one draw needn't show every extreme that they name: `expert_ids`: each row names 8 different experts; in every section and micro-batch one expert below 2 is named by every row. `keep_mask`: 1 only where the expert named is below 2; in one block of 128 rows no expert has more than 4 kept choices, and in every section and micro-batch one expert has exactly 4 in every block. `slot_pos`: kept choices of one block naming the same expert hold different slots; 0 where keep_mask is 0.
All inputs are finite; a program needn't handle non-finite values.
Results may differ from the reference program's by a relative error of at most 0.005.
Values may be sent and summed in bfloat16 or wider, within the bound.
A program may use at most 64 MiB of HBM per device.

```python
import jax
import jax.numpy as jnp
from jax import lax

D = 3584
FE = 1024
FS = 1024
SPECIALIST_COUNT = 256
TOPK = 8
TOK_DEV = 128
SECTIONS = 4
EXPERTS = 2
TOKENS = 512
CAP = 4
N_EXPERT = 4
N_TENSOR = 2


def routing_tables(key):
    base = jax.random.fold_in(key, 29)
    key_score, key_lean, key_force, key_order = jax.random.split(base, 4)
    blocks = TOKENS // TOK_DEV
    choices = TOK_DEV * TOPK
    gating_logits = jax.random.randint(key_score, (2, SECTIONS, TOKENS, SPECIALIST_COUNT), 0, 65536)
    preference_offset = jax.random.randint(key_lean, (SPECIALIST_COUNT,), 0, 3) * 32768
    imposed_selection = jax.random.randint(key_force, (2, SECTIONS, 1, 1), 0, EXPERTS)
    uniform_draws = jnp.arange(SPECIALIST_COUNT, dtype=jnp.int32)
    extra_increment = jnp.where(uniform_draws == imposed_selection, 1 << 20, 0)
    sorted_specialists = (gating_logits + preference_offset + extra_increment) * SPECIALIST_COUNT + uniform_draws
    _, chosen = lax.top_k(sorted_specialists, TOPK)
    chosen = chosen.astype(jnp.int32)
    lined = chosen.reshape(2 * SECTIONS * blocks, choices)
    onehot = (lined[:, :, None] == jnp.arange(EXPERTS, dtype=jnp.int32)).astype(jnp.int32)
    order_keys = jax.random.split(key_order, 2 * SECTIONS * blocks)
    order = jax.vmap(lambda single: jax.random.permutation(single, choices))(order_keys).astype(jnp.int32)
    placed = jnp.take_along_axis(onehot, order[:, :, None], axis=1)
    before = jnp.cumsum(placed, axis=1) - placed
    rank_sorted = jnp.sum(before * placed, axis=-1)
    inverse = jnp.argsort(order, axis=1, stable=True)
    position = jnp.take_along_axis(rank_sorted, inverse, axis=1)
    kept = (lined < EXPERTS) & (position < CAP)
    slots = jnp.where(kept, position, 0)
    target_shape = (2, SECTIONS, TOKENS, TOPK)
    return (chosen, kept.astype(jnp.int32).reshape(target_shape), slots.astype(jnp.int32).reshape(target_shape))


def draw_expert_ids(key, part):
    return routing_tables(key)[0]


def draw_keep_mask(key, part):
    return routing_tables(key)[1]


def draw_slot_pos(key, part):
    return routing_tables(key)[2]


def with_ends(drawn, own_key, low, largest):
    place = [jax.random.randint(jax.random.fold_in(own_key, axis), (), 0, length) for axis, length in enumerate(drawn.shape)]
    main_axis = drawn.shape.index(max(drawn.shape))
    next_to = place[:main_axis] + [(place[main_axis] + 1) % drawn.shape[main_axis]] + place[main_axis + 1:]
    return drawn.at[tuple(place)].set(low).at[tuple(next_to)].set(largest)


def block_scale(stream_key, extent, cuts, smallest, top_value):
    factor_of = 1.0
    for axis_at, blocks in cuts:
        draws = jax.random.uniform(jax.random.fold_in(jax.random.fold_in(stream_key, 6), axis_at), (blocks,), jnp.float32, smallest / len(cuts), top_value / len(cuts))
        factor_of = factor_of * jnp.repeat(jnp.exp(draws), extent[axis_at] // blocks).reshape((-1,) + (1,) * (len(extent) - 1 - axis_at))
    return factor_of


def scatter_about(own_key, dims, width, bound, shards=(), kind=jnp.bfloat16):
    drawn = jax.random.normal(own_key, dims, jnp.float32) * width
    if len(shards) > 0:
        drawn = block_scale(own_key, dims, shards, -0.22, 0.18) * drawn
    return jnp.clip(drawn, min=-bound, max=bound).astype(kind)


def setup_inputs(seed: int = 0) -> dict:
    key_of = jax.random.split(jax.random.key(seed), 14)
    return {
        "inputs_prev": scatter_about(key_of[0], (SECTIONS, TOKENS, D), 1.0, 6.0, ((0, 4), (1, 4), (2, 2))),
        "cotangent_next": scatter_about(key_of[1], (SECTIONS, TOKENS, D), 1.0, 6.0, ((0, 4), (1, 4), (2, 2))),
        "saved_input": scatter_about(key_of[2], (SECTIONS, TOKENS, D), 1.0, 6.0, ((0, 4), (1, 4), (2, 2))),
        "expert_ids": draw_expert_ids(jax.random.fold_in(key_of[13], 71), 0),
        "keep_mask": draw_keep_mask(jax.random.fold_in(key_of[13], 71), 0),
        "slot_pos": draw_slot_pos(jax.random.fold_in(key_of[13], 71), 0),
        "weight_q": with_ends(jax.random.randint(key_of[6], (2, SECTIONS, TOKENS, TOPK), 1, 4096), jax.random.fold_in(key_of[6], 1), 1, 4095).astype(jnp.int32),
        "gate_routed": scatter_about(key_of[7], (SECTIONS, N_EXPERT, D, FE // 2), D ** -0.5, 0.09375, ((0, 4), (1, 4), (3, 2))),
        "up_routed": scatter_about(key_of[8], (SECTIONS, N_EXPERT, D, FE // 2), D ** -0.5, 0.09375, ((0, 4), (1, 4), (3, 2))),
        "down_routed": scatter_about(key_of[9], (SECTIONS, N_EXPERT, FE // 2, D), FE ** -0.5, 0.1875, ((0, 4), (1, 4), (2, 2))),
        "gate_shared": scatter_about(key_of[10], (SECTIONS, D, FS), D ** -0.5, 0.09375, ((0, 4), (2, 2))),
        "up_shared": scatter_about(key_of[11], (SECTIONS, D, FS), D ** -0.5, 0.09375, ((0, 4), (2, 2))),
        "down_shared": scatter_about(key_of[12], (SECTIONS, FS, D), FS ** -0.5, 0.1875, ((0, 4), (1, 2))),
    }


def swish(values):
    return values * jax.nn.sigmoid(values)


def swish_slope(values):
    logistic = jax.nn.sigmoid(values)
    return logistic * (1.0 + values * (1.0 - logistic))


def slot_plan(choice_ids, kept_flags, slot_index, weight_levels, experts_here, capacity):
    total_slots = experts_here * capacity
    target = jnp.where(kept_flags > 0, choice_ids * capacity + slot_index, total_slots).reshape(-1).astype(jnp.int32)
    source = jnp.broadcast_to(jnp.arange(choice_ids.shape[0], dtype=jnp.int32)[:, None], choice_ids.shape).reshape(-1)
    slot_token = jnp.zeros((total_slots,), jnp.int32).at[target].set(source, mode="drop")
    levels = (weight_levels.astype(jnp.float32) / 4096.0).reshape(-1)
    slot_weight = jnp.zeros((total_slots,), jnp.float32).at[target].set(levels, mode="drop")
    slot_live = jnp.zeros((total_slots,), jnp.float32).at[target].set(1.0, mode="drop")
    return slot_token, slot_weight, slot_live


def contract_last(left, right):
    return lax.dot_general(left, right, (((1,), (1,)), ((), ())), preferred_element_type=jnp.float32)


def expert_pass(packed):
    rows_in, rows_saved, rows_cot, gate_w, up_w, down_w = packed
    part_width = FE // (2 * N_TENSOR)
    gate_pre = jnp.dot(rows_in, gate_w, preferred_element_type=jnp.float32)
    up_pre = jnp.dot(rows_in, up_w, preferred_element_type=jnp.float32)
    hidden = (swish(gate_pre) * up_pre).astype(jnp.bfloat16)
    gate_back = jnp.dot(rows_saved, gate_w, preferred_element_type=jnp.float32)
    up_back = jnp.dot(rows_saved, up_w, preferred_element_type=jnp.float32)
    grad_hidden = contract_last(rows_cot, down_w)
    grad_gate = (grad_hidden * up_back * swish_slope(gate_back)).astype(jnp.bfloat16)
    grad_up = (grad_hidden * swish(gate_back)).astype(jnp.bfloat16)
    result = jnp.zeros((rows_in.shape[0], rows_in.shape[1]), jnp.float32)
    grad_rows = jnp.zeros((rows_in.shape[0], rows_in.shape[1]), jnp.float32)
    for group_j in range(FE // part_width):
        lower = group_j * part_width
        upper = lower + part_width
        piece_out = jnp.dot(hidden[:, lower:upper], down_w[lower:upper], preferred_element_type=jnp.float32)
        result = result + piece_out.astype(jnp.bfloat16).astype(jnp.float32)
        piece_grad = contract_last(grad_gate[:, lower:upper], gate_w[:, lower:upper]) + contract_last(grad_up[:, lower:upper], up_w[:, lower:upper])
        grad_rows = grad_rows + piece_grad.astype(jnp.bfloat16).astype(jnp.float32)
    return result, grad_rows


def shared_pass(full_in, full_saved, full_cot, gate_w, up_w, down_w):
    gate_pre = jnp.dot(full_in, gate_w, preferred_element_type=jnp.float32)
    up_pre = jnp.dot(full_in, up_w, preferred_element_type=jnp.float32)
    hidden = (swish(gate_pre) * up_pre).astype(jnp.bfloat16)
    shared_out = jnp.dot(hidden, down_w, preferred_element_type=jnp.float32)
    gate_back = jnp.dot(full_saved, gate_w, preferred_element_type=jnp.float32)
    up_back = jnp.dot(full_saved, up_w, preferred_element_type=jnp.float32)
    grad_hidden = contract_last(full_cot, down_w)
    grad_gate = (grad_hidden * up_back * swish_slope(gate_back)).astype(jnp.bfloat16)
    grad_up = (grad_hidden * swish(gate_back)).astype(jnp.bfloat16)
    shared_grad = contract_last(grad_gate, gate_w) + contract_last(grad_up, up_w)
    return shared_out, shared_grad


def one_section(packed):
    (section_in, section_saved, section_cot, ids_fwd, keep_fwd, slot_fwd, level_fwd, ids_bwd, keep_bwd, slot_bwd, level_bwd,
     gate_section, up_section, down_section, shared_gate, shared_up, shared_down) = packed
    blocks = TOKENS // TOK_DEV
    half_width = FE // 2

    def plan_all(ids_all, keep_all, slot_all, level_all):
        return jax.vmap(lambda a, b, c, e: slot_plan(a, b, c, e, EXPERTS, CAP))(
            ids_all.reshape(blocks, TOK_DEV, TOPK), keep_all.reshape(blocks, TOK_DEV, TOPK),
            slot_all.reshape(blocks, TOK_DEV, TOPK), level_all.reshape(blocks, TOK_DEV, TOPK))

    token_f, weight_f, live_f = plan_all(ids_fwd, keep_fwd, slot_fwd, level_fwd)
    token_b, weight_b, live_b = plan_all(ids_bwd, keep_bwd, slot_bwd, level_bwd)

    def pick(values, tokens_at, live_at):
        return jnp.where(live_at[:, None] > 0, values[tokens_at], jnp.zeros((), values.dtype))

    def scaled(values, tokens_at, weight_at):
        return (weight_at[:, None] * values[tokens_at].astype(jnp.float32)).astype(jnp.bfloat16)

    rows_in = jax.vmap(pick)(section_in.reshape(blocks, TOK_DEV, D), token_f, live_f)
    rows_saved = jax.vmap(pick)(section_saved.reshape(blocks, TOK_DEV, D), token_b, live_b)
    rows_cot = jax.vmap(scaled)(section_cot.reshape(blocks, TOK_DEV, D), token_b, weight_b)

    def to_expert(rows):
        return rows.reshape(blocks, EXPERTS, CAP, D).transpose(1, 0, 2, 3).reshape(EXPERTS, blocks * CAP, D)

    def from_expert(rows):
        return rows.reshape(EXPERTS, blocks, CAP, D).transpose(1, 0, 2, 3).reshape(blocks, EXPERTS * CAP, D)

    gate_full = gate_section.reshape(EXPERTS, 2, D, half_width).transpose(0, 2, 1, 3).reshape(EXPERTS, D, FE)
    up_full = up_section.reshape(EXPERTS, 2, D, half_width).transpose(0, 2, 1, 3).reshape(EXPERTS, D, FE)
    down_full = down_section.reshape(EXPERTS, FE, D)
    expert_out, expert_grad = lax.map(expert_pass, (to_expert(rows_in), to_expert(rows_saved), to_expert(rows_cot), gate_full, up_full, down_full))

    def combine(tokens_at, weight_at, rows):
        return jnp.zeros((TOK_DEV, D), jnp.float32).at[tokens_at].add(weight_at[:, None] * rows)

    routed_out = jax.vmap(combine)(token_f, weight_f, from_expert(expert_out)).reshape(TOKENS, D)
    routed_grad = jax.vmap(combine)(token_b, live_b, from_expert(expert_grad)).reshape(TOKENS, D)
    shared_out, shared_grad = shared_pass(section_in, section_saved, section_cot, shared_gate, shared_up, shared_down)
    return (shared_out + routed_out).astype(jnp.bfloat16), (shared_grad + routed_grad).astype(jnp.bfloat16)


def reference(inputs_prev, cotangent_next, saved_input, expert_ids, keep_mask, slot_pos, weight_q, gate_routed, up_routed, down_routed, gate_shared, up_shared, down_shared):
    forward_in = jnp.roll(inputs_prev, 1, axis=0)
    backward_in = jnp.roll(cotangent_next, -1, axis=0)
    out_act, in_grad = lax.map(one_section, (forward_in, saved_input, backward_in,
                                           expert_ids[0], keep_mask[0], slot_pos[0], weight_q[0],
                                           expert_ids[1], keep_mask[1], slot_pos[1], weight_q[1],
                                           gate_routed, up_routed, down_routed, gate_shared, up_shared, down_shared))
    return out_act, in_grad
```

```python
import functools

import jax
import jax.numpy as jnp
from jax import lax
from jax.experimental import pallas as pl
from jax.experimental.pallas import tpu as pltpu
from jax.sharding import PartitionSpec as P

MESH = pl.DeviceIdType.MESH
F32 = jnp.float32
BF16 = jnp.bfloat16
BLOCK = 8
LAST_COT = 2
INPUT_GATE = 4


def swish(values):
    return values * jax.nn.sigmoid(values)


def swish_slope(values):
    logistic = jax.nn.sigmoid(values)
    return logistic * (1.0 + values * (1.0 - logistic))


def dot(left, right):
    return jnp.dot(left, right, preferred_element_type=F32)


def contract_last(left, right):
    return lax.dot_general(left, right, (((1,), (1,)), ((), ())), preferred_element_type=F32)


def chunk_of(width):
    return 256 if width % 256 == 0 else 128


def kernel(
    sizes,
    x_hbm, c_hbm, saved_hbm, ids_hbm, keep_hbm, slot_hbm, level_hbm,
    gate_r_hbm, up_r_hbm, down_r_hbm, gate_s_hbm, up_s_hbm, down_s_hbm,
    out_ref, grad_ref,
    gate_r, up_r, down_r, gate_s, up_s, down_s, down_peer,
    tables, tables_next, x_own, c_own, full_x, full_c, full_s,
    a_saved, b_saved, gate_pre, up_pre, grad_hid, hidden, hidden_peer, grad_gate, grad_up,
    a_routed, b_routed,
    send_s, send_c, send_x, held_x, recv_s, recv_c, recv_x, rows,
    back_send_g, back_recv_g, back_send_o, back_recv_o, back_rows,
    part_grad, peer_grad, out_sum,
    weight_sem, table_sem, local_sem,
    next_send, next_recv, saved_send, saved_recv, down_send, down_recv,
    c_send, c_recv, x_send, x_recv, cf_send, cf_recv, xf_send, xf_recv,
    rs_send, rs_recv, rc_send, rc_recv, rx_send, rx_recv, pick_send, pick_recv,
    bg_send, bg_recv, bo_send, bo_recv, part_send, part_recv, hid_send, hid_recv,
):
    n_pipe, ne, nt, capacity = sizes
    tokens, width = x_own.shape
    features = width * nt
    blocks = send_s.shape[0]
    me_p, me_e, me_t = lax.axis_index("pipe"), lax.axis_index("expert"), lax.axis_index("tensor")
    nxt, prv = lax.rem(me_p + 1, n_pipe), lax.rem(me_p + n_pipe - 1, n_pipe)
    my_cols = pl.ds(pl.multiple_of(me_t * width, 128), width)
    cw = chunk_of(width)
    chunks = width // cw
    started = []

    def peer_t(step):
        return lax.rem(me_t + step, nt)

    def peer_e(step):
        return lax.rem(me_e + step, ne)

    def source_t(step):
        return lax.rem(me_t + nt - step, nt)

    def remote(src, dst, ssem, rsem, device):
        copy = pltpu.make_async_remote_copy(
            src_ref=src, dst_ref=dst, send_sem=ssem, recv_sem=rsem,
            device_id=device, device_id_type=MESH,
        )
        copy.start()
        started.append(copy)
        return copy

    def load(src, dst, sem):
        copy = pltpu.make_async_copy(src, dst, sem)
        copy.start()
        return copy

    def local_cols(n):
        return pl.ds(pl.multiple_of(n * cw, 128), cw)

    def cols_of(part, n):
        return pl.ds(pl.multiple_of(part * width + n * cw, 128), cw)

    table_loads = [
        load(src, tables.at[a], table_sem.at[a])
        for a, src in enumerate((ids_hbm, keep_hbm, slot_hbm, level_hbm))
    ]
    c_load = load(c_hbm, c_own, local_sem.at[0])
    saved_load = load(saved_hbm, full_s.at[:, my_cols], local_sem.at[1])
    x_load = load(x_hbm, x_own, local_sem.at[2])
    gate_s_load = load(gate_s_hbm, gate_s, weight_sem.at[0])
    up_s_load = load(up_s_hbm, up_s, weight_sem.at[1])
    gate_r_load = load(gate_r_hbm, gate_r, weight_sem.at[2])
    up_r_load = load(up_r_hbm, up_r, weight_sem.at[3])
    down_s_load = load(down_s_hbm, down_s, weight_sem.at[4])
    down_r_load = load(down_r_hbm, down_r, weight_sem.at[5])

    barrier = pltpu.get_barrier_semaphore()
    greeted = [{"pipe": nxt}, {"pipe": prv}]
    for se in range(ne):
        for st in range(nt):
            if se or st:
                greeted.append({"expert": peer_e(se), "tensor": peer_t(st)})
    for device in greeted:
        pl.semaphore_signal(barrier, inc=1, device_id=device, device_id_type=MESH)
    pl.semaphore_wait(barrier, len(greeted))

    for copy in table_loads:
        copy.wait()
    next_copies = [
        remote(tables.at[a, 0], tables_next.at[a], next_send.at[a], next_recv.at[a], {"pipe": prv})
        for a in range(3)
    ]

    def send_cot(n):
        return remote(
            c_own.at[:, local_cols(n)], full_c.at[:, cols_of(me_t, n)],
            c_send.at[n], c_recv.at[n], {"pipe": prv},
        )

    def send_in(n):
        return remote(
            x_own.at[:, local_cols(n)], full_x.at[:, cols_of(me_t, n)],
            x_send.at[n], x_recv.at[n], {"pipe": nxt},
        )

    c_load.wait()
    c_copies = [send_cot(n) for n in range(chunks - LAST_COT)]
    saved_load.wait()
    saved_copies = [
        remote(
            full_s.at[:, my_cols], full_s.at[:, my_cols], saved_send.at[st - 1],
            saved_recv.at[st - 1], {"tensor": peer_t(st)},
        )
        for st in range(1, nt)
    ]
    down_copies = []
    for st in range(1, nt):
        to = peer_t(st)
        down_copies.append(remote(
            down_s_hbm.at[:, pl.ds(pl.multiple_of(to * width, 128), width)], down_peer.at[st - 1],
            down_send.at[st - 1], down_recv.at[st - 1], {"tensor": to},
        ))

    def table(target, values, slots_at):
        total = jnp.zeros((slots_at.shape[0], tokens), jnp.int32)
        for k in range(target.shape[0]):
            total = total + jnp.where(target[k:k + 1] == slots_at, values[k:k + 1], 0)
        return total

    def targets(ids, keep, slot):
        return jnp.where(keep > 0, ids * capacity + slot, -1)

    target_f = targets(tables[0, 0], tables[1, 0], tables[2, 0])
    target_b = targets(tables[0, 1], tables[1, 1], tables[2, 1])
    level_f, level_b = tables[3, 0], tables[3, 1]
    used = max(16, blocks * BLOCK)
    place = lax.broadcasted_iota(jnp.int32, (used, tokens), 0)
    ones = jnp.ones(target_f.shape, jnp.int32)
    pick_b = table(target_b, ones, place).astype(F32).astype(BF16)
    scale_b = jnp.sum(table(target_b, level_b, place).astype(F32), axis=1, keepdims=True) / 4096.0

    def exchange(source_of, landing, ssem, rsem):
        copies = []
        for se in range(ne):
            for st in range(nt):
                if se or st:
                    to_e, n = peer_e(se), se * nt + st - 1
                    copies.append(remote(
                        source_of(to_e), landing.at[me_e, :, my_cols], ssem.at[n], rsem.at[n],
                        {"expert": to_e, "tensor": peer_t(st)},
                    ))
        return copies

    def block_of(e):
        return lax.div(lax.div(e, 2) * capacity, BLOCK)

    def keep_own(buffer, landing):
        landing[me_e, :, my_cols] = buffer[block_of(me_e)]

    def gather_rows(landing):
        for i in range(0, ne, 2):
            both = jnp.concatenate(
                (landing[i].astype(F32), landing[i + 1].astype(F32)), axis=0
            )
            rows[i * BLOCK:(i + 2) * BLOCK, :] = both.astype(BF16)

    def pick_rows(picks, scale, read, buffer, n):
        picked = dot(picks, read(n))
        if scale is not None:
            picked = picked * scale
        for b in range(blocks):
            buffer[b, :, local_cols(n)] = picked[b * BLOCK:(b + 1) * BLOCK].astype(BF16)

    def saved_rows(n, carry):
        pick_rows(pick_b, None, lambda m: full_s[:, cols_of(me_t, m)], send_s, n)
        return carry

    lax.fori_loop(0, chunks, saved_rows, 0)
    saved_row_copies = exchange(lambda e: send_s.at[block_of(e)], recv_s, rs_send, rs_recv)
    keep_own(send_s, recv_s)

    for copy in saved_copies:
        copy.wait_recv()
    gate_s_load.wait()
    up_s_load.wait()
    cs = chunk_of(gate_s.shape[1])

    def shared_saved(n, carry):
        cols = pl.ds(pl.multiple_of(n * cs, 128), cs)
        gate_back = dot(full_s[...], gate_s[:, cols])
        up_back = dot(full_s[...], up_s[:, cols])
        a_saved[:, cols] = up_back * swish_slope(gate_back)
        b_saved[:, cols] = swish(gate_back)
        return carry

    lax.fori_loop(0, gate_s.shape[1] // cs, shared_saved, 0)

    for copy in next_copies:
        copy.wait_recv()
    x_load.wait()
    target_n = targets(tables_next[0], tables_next[1], tables_next[2])
    pick_n = table(target_n, ones, place).astype(F32).astype(BF16)

    def input_rows(n, carry):
        pick_rows(pick_n, None, lambda m: x_own[:, local_cols(m)], send_x, n)
        return carry

    lax.fori_loop(0, chunks, input_rows, 0)
    picked_copy = remote(send_x, held_x, pick_send, pick_recv, {"pipe": nxt})
    c_copies += [send_cot(n) for n in range(chunks - LAST_COT, chunks)]

    for copy in saved_row_copies:
        copy.wait_recv()
    gather_rows(recv_s)
    gate_r_load.wait()
    up_r_load.wait()
    gate_back = dot(rows[...], gate_r[...])
    a_routed[...] = dot(rows[...], up_r[...]) * swish_slope(gate_back)
    b_routed[...] = swish(gate_back)

    down_s_load.wait()

    def forward(held, n, ssem, rsem):
        cols = cols_of(me_t, n)
        return [
            remote(
                held.at[:, cols], held.at[:, cols], ssem.at[n, st - 1], rsem.at[n, st - 1],
                {"tensor": peer_t(st)},
            )
            for st in range(1, nt)
        ]

    def add_cot(part, n, first=False):
        cols = cols_of(part, n)
        piece = contract_last(full_c[:, cols], down_s[:, cols])
        grad_hid[...] = piece if first else grad_hid[...] + piece

    def add_forwarded(copies, n, add):
        for st in range(1, nt):
            copies[st - 1].wait_recv()
            add(source_t(st), n)

    x_copies = []
    cf_copies = []
    for n in range(chunks):
        c_copies[n].wait_recv()
        cf_copies.append(forward(full_c, n, cf_send, cf_recv))
        if n == INPUT_GATE:
            x_copies = [send_in(m) for m in range(chunks)]
        pick_rows(pick_b, scale_b, lambda m: full_c[:, cols_of(me_t, m)], send_c, n)
        if n == chunks - 1:
            cot_row_copies = exchange(lambda e: send_c.at[block_of(e)], recv_c, rc_send, rc_recv)
        add_cot(me_t, n, first=n == 0)
        if n:
            add_forwarded(cf_copies[n - 1], n - 1, add_cot)
    keep_own(send_c, recv_c)
    add_forwarded(cf_copies[chunks - 1], chunks - 1, add_cot)

    grad_gate[...] = (grad_hid[...] * a_saved[...]).astype(BF16)
    grad_up[...] = (grad_hid[...] * b_saved[...]).astype(BF16)
    part_copies = []
    for st in list(range(1, nt)) + [0]:
        to = peer_t(st)

        def shared_back(n, carry, st=st, to=to):
            cols = cols_of(to, n)
            part_grad[st, :, local_cols(n)] = (
                contract_last(grad_gate[...], gate_s[cols, :])
                + contract_last(grad_up[...], up_s[cols, :])
            )
            return carry

        lax.fori_loop(0, chunks, shared_back, 0)
        if st:
            part_copies.append(remote(
                part_grad.at[st], peer_grad.at[st - 1], part_send.at[st - 1],
                part_recv.at[st - 1], {"tensor": to},
            ))

    picked_copy.wait_recv()
    input_row_copies = exchange(lambda e: held_x.at[block_of(e)], recv_x, rx_send, rx_recv)
    keep_own(held_x, recv_x)

    def send_back(total_of, buffer, landing, ssem, rsem):
        copies = []
        for st in list(range(1, nt)) + [0]:
            to_t = peer_t(st)

            def second(n, carry, to_t=to_t):
                total = total_of(cols_of(to_t, n))
                for i in range(ne):
                    buffer[i, to_t, :, local_cols(n)] = (
                        total[i * BLOCK:(i + 1) * BLOCK].astype(BF16)
                    )
                return carry

            lax.fori_loop(0, chunks, second, 0)
            for se in range(ne):
                if se or st:
                    to_e, n = peer_e(se), se * nt + st - 1
                    copies.append(remote(
                        buffer.at[to_e, to_t], landing.at[me_e, me_t], ssem.at[n], rsem.at[n],
                        {"expert": to_e, "tensor": to_t},
                    ))
        landing[me_e, me_t] = buffer[me_e, me_t]
        return copies

    for copy in cot_row_copies:
        copy.wait_recv()
    gather_rows(recv_c)
    down_r_load.wait()
    grad_back = contract_last(rows[...], down_r[...])
    gate_grad_r = (grad_back * a_routed[...]).astype(BF16)
    up_grad_r = (grad_back * b_routed[...]).astype(BF16)
    grad_back_copies = send_back(
        lambda cols: contract_last(gate_grad_r, gate_r[cols, :])
        + contract_last(up_grad_r, up_r[cols, :]),
        back_send_g, back_recv_g, bg_send, bg_recv,
    )

    for copy in input_row_copies:
        copy.wait_recv()
    gather_rows(recv_x)
    gate_fwd = dot(rows[...], gate_r[...])
    hidden_r = (swish(gate_fwd) * dot(rows[...], up_r[...])).astype(BF16)
    out_back_copies = send_back(
        lambda cols: dot(hidden_r, down_r[:, cols]), back_send_o, back_recv_o, bo_send, bo_recv
    )

    parts = ne * nt * BLOCK
    place_b = lax.broadcasted_iota(jnp.int32, (parts, tokens), 0)
    inside = lax.rem(place_b, BLOCK)
    expert = lax.div(lax.div(place_b, nt * BLOCK), 2)
    own = lax.div(inside, capacity) == lax.rem(expert, BLOCK // capacity)
    slots = jnp.where(own, expert * capacity + lax.rem(inside, capacity), -2)

    def gather_back(landing):
        for i in range(0, ne * nt, 2):
            first, second = divmod(i, nt), divmod(i + 1, nt)
            both = jnp.concatenate((landing[first].astype(F32), landing[second].astype(F32)), axis=0)
            back_rows[i * BLOCK:(i + 2) * BLOCK, :] = both.astype(BF16)

    def finish_grad():
        factor = table(target_b, ones, slots).astype(F32).T.astype(BF16)
        for copy in grad_back_copies:
            copy.wait_recv()
        gather_back(back_recv_g)
        for copy in part_copies:
            copy.wait_recv()

        def body(n, carry):
            at = local_cols(n)
            total = part_grad[0, :, at] + dot(factor, back_rows[:, at])
            for st in range(1, nt):
                total = total + peer_grad[st - 1, :, at]
            grad_ref[:, at] = total.astype(BF16)
            return carry

        lax.fori_loop(0, chunks, body, 0)

    def start_out():
        level = table(target_f, level_f, slots)
        high = lax.div(level, 64)
        low = level - high * 64
        factor_high = (high.astype(F32) / 64.0).T.astype(BF16)
        factor_low = (low.astype(F32) / 4096.0).T.astype(BF16)
        for copy in out_back_copies:
            copy.wait_recv()
        gather_back(back_recv_o)

        def body(n, carry):
            at = local_cols(n)
            out_sum[:, at] = dot(factor_high, back_rows[:, at]) + dot(factor_low, back_rows[:, at])
            return carry

        lax.fori_loop(0, chunks, body, 0)

    def add_in(part, n, first=False):
        cols = cols_of(part, n)
        piece = full_x[:, cols]
        gate_piece, up_piece = dot(piece, gate_s[cols, :]), dot(piece, up_s[cols, :])
        gate_pre[...] = gate_piece if first else gate_pre[...] + gate_piece
        up_pre[...] = up_piece if first else up_pre[...] + up_piece

    xf_copies = []
    for n in range(chunks):
        if n == chunks - 2:
            finish_grad()
        if n == chunks - 1:
            start_out()
            for copy in down_copies:
                copy.wait_recv()
        x_copies[n].wait_recv()
        xf_copies.append(forward(full_x, n, xf_send, xf_recv))
        add_in(me_t, n, first=n == 0)
        if n:
            add_forwarded(xf_copies[n - 1], n - 1, add_in)
    add_forwarded(xf_copies[chunks - 1], chunks - 1, add_in)

    hidden[...] = (swish(gate_pre[...]) * up_pre[...]).astype(BF16)
    hid_copies = [
        remote(
            hidden, hidden_peer.at[st - 1], hid_send.at[st - 1], hid_recv.at[st - 1],
            {"tensor": peer_t(st)},
        )
        for st in range(1, nt)
    ]

    def own_part(n, carry):
        at = local_cols(n)
        out_sum[:, at] = out_sum[:, at] + dot(hidden[...], down_s[:, cols_of(me_t, n)])
        return carry

    lax.fori_loop(0, chunks, own_part, 0)
    for copy in hid_copies:
        copy.wait_recv()

    def peer_part(n, carry):
        at = local_cols(n)
        total = out_sum[:, at]
        for st in range(1, nt):
            total = total + dot(hidden_peer[st - 1], down_peer[st - 1, :, at])
        out_ref[:, at] = total.astype(BF16)
        return carry

    lax.fori_loop(0, chunks, peer_part, 0)

    for copy in started:
        copy.wait_send()


def store(out, grad, out_hbm, grad_hbm, sem):
    first = pltpu.make_async_copy(out, out_hbm, sem.at[0])
    second = pltpu.make_async_copy(grad, grad_hbm, sem.at[1])
    first.start()
    second.start()
    first.wait()
    second.wait()


def lanes_last(choices):
    return jnp.swapaxes(choices[:, 0], 1, 2)


def in_hbm(values):
    return pltpu.with_memory_space_constraint(values, pltpu.HBM)


def local(
    inputs_prev, cotangent_next, saved_input, expert_ids, keep_mask, slot_pos, weight_q,
    gate_routed, up_routed, down_routed, gate_shared, up_shared, down_shared,
):
    n_pipe, ne, nt = lax.axis_size("pipe"), lax.axis_size("expert"), lax.axis_size("tensor")
    tokens, width = inputs_prev.shape[1:]
    topk = expert_ids.shape[3]
    features = width * nt
    capacity = tokens // 32
    experts = ne // 2
    blocks = -(-experts * capacity // BLOCK)
    fr, fs = gate_routed.shape[3], gate_shared.shape[2]
    chunks = width // chunk_of(width)
    peers = ne * nt - 1
    vmem = pl.BlockSpec(memory_space=pltpu.VMEM)
    hbm = pl.BlockSpec(memory_space=pl.ANY)
    dma = pltpu.SemaphoreType.DMA
    shape = pltpu.VMEM((tokens, width), BF16)
    out, grad = pl.pallas_call(
        functools.partial(kernel, (n_pipe, ne, nt, capacity)),
        out_shape=(shape, shape),
        in_specs=[hbm] * 13,
        out_specs=(vmem, vmem),
        scratch_shapes=[
            pltpu.VMEM((features, fr), BF16),
            pltpu.VMEM((features, fr), BF16),
            pltpu.VMEM((fr, features), BF16),
            pltpu.VMEM((features, fs), BF16),
            pltpu.VMEM((features, fs), BF16),
            pltpu.VMEM((fs, features), BF16),
            pltpu.VMEM((nt - 1, fs, width), BF16),
            pltpu.VMEM((4, 2, topk, tokens), jnp.int32),
            pltpu.VMEM((3, topk, tokens), jnp.int32),
            pltpu.VMEM((tokens, width), BF16),
            pltpu.VMEM((tokens, width), BF16),
            pltpu.VMEM((tokens, features), BF16),
            pltpu.VMEM((tokens, features), BF16),
            pltpu.VMEM((tokens, features), BF16),
            pltpu.VMEM((tokens, fs), F32),
            pltpu.VMEM((tokens, fs), F32),
            pltpu.VMEM((tokens, fs), F32),
            pltpu.VMEM((tokens, fs), F32),
            pltpu.VMEM((tokens, fs), F32),
            pltpu.VMEM((tokens, fs), BF16),
            pltpu.VMEM((nt - 1, tokens, fs), BF16),
            pltpu.VMEM((tokens, fs), BF16),
            pltpu.VMEM((tokens, fs), BF16),
            pltpu.VMEM((ne * BLOCK, fr), F32),
            pltpu.VMEM((ne * BLOCK, fr), F32),
            pltpu.VMEM((blocks, BLOCK, width), BF16),
            pltpu.VMEM((blocks, BLOCK, width), BF16),
            pltpu.VMEM((blocks, BLOCK, width), BF16),
            pltpu.VMEM((blocks, BLOCK, width), BF16),
            pltpu.VMEM((ne, BLOCK, features), BF16),
            pltpu.VMEM((ne, BLOCK, features), BF16),
            pltpu.VMEM((ne, BLOCK, features), BF16),
            pltpu.VMEM((ne * BLOCK, features), BF16),
            pltpu.VMEM((ne, nt, BLOCK, width), BF16),
            pltpu.VMEM((ne, nt, BLOCK, width), BF16),
            pltpu.VMEM((ne, nt, BLOCK, width), BF16),
            pltpu.VMEM((ne, nt, BLOCK, width), BF16),
            pltpu.VMEM((ne * nt * BLOCK, width), BF16),
            pltpu.VMEM((nt, tokens, width), F32),
            pltpu.VMEM((nt - 1, tokens, width), F32),
            pltpu.VMEM((tokens, width), F32),
            dma((6,)), dma((4,)), dma((3,)),
            dma((3,)), dma((3,)),
            dma((nt - 1,)), dma((nt - 1,)), dma((nt - 1,)), dma((nt - 1,)),
            dma((chunks,)), dma((chunks,)), dma((chunks,)), dma((chunks,)),
            dma((chunks, nt - 1)), dma((chunks, nt - 1)),
            dma((chunks, nt - 1)), dma((chunks, nt - 1)),
            dma((peers,)), dma((peers,)), dma((peers,)), dma((peers,)),
            dma((peers,)), dma((peers,)), dma, dma,
            dma((peers,)), dma((peers,)), dma((peers,)), dma((peers,)),
            dma((nt - 1,)), dma((nt - 1,)), dma((nt - 1,)), dma((nt - 1,)),
        ],
        compiler_params=pltpu.CompilerParams(
            collective_id=0, has_side_effects=True, vmem_limit_bytes=60 * 1024 * 1024
        ),
        name="moe_step",
    )(
        *(in_hbm(v) for v in (
            inputs_prev[0], cotangent_next[0], saved_input[0],
            *(lanes_last(v) for v in (expert_ids, keep_mask, slot_pos, weight_q)),
            gate_routed[0, 0], up_routed[0, 0], down_routed[0, 0],
            gate_shared[0], up_shared[0], down_shared[0],
        ))
    )
    result = jax.ShapeDtypeStruct((tokens, width), BF16)
    out, grad = pl.pallas_call(
        store,
        out_shape=(result, result),
        in_specs=[vmem] * 2,
        out_specs=(hbm, hbm),
        scratch_shapes=[dma((2,))],
        compiler_params=pltpu.CompilerParams(vmem_limit_bytes=2 * 1024 * 1024),
        name="store_out",
    )(*(pltpu.with_memory_space_constraint(v, pltpu.VMEM) for v in (out, grad)))
    return out[None], grad[None]


def solution(mesh):
    return jax.shard_map(
        local,
        mesh=mesh,
        in_specs=(
            P("pipe", "expert", "tensor"),
            P("pipe", "expert", "tensor"),
            P("pipe", "expert", "tensor"),
            P(None, "pipe", "expert", None),
            P(None, "pipe", "expert", None),
            P(None, "pipe", "expert", None),
            P(None, "pipe", "expert", None),
            P("pipe", "expert", None, "tensor"),
            P("pipe", "expert", None, "tensor"),
            P("pipe", "expert", "tensor", None),
            P("pipe", None, "tensor"),
            P("pipe", None, "tensor"),
            P("pipe", "tensor", None),
        ),
        out_specs=(P("pipe", "expert", "tensor"), P("pipe", "expert", "tensor")),
        check_vma=False,
    )
```

```python
import functools

import jax
import jax.numpy as jnp
from jax import lax
from jax.experimental import pallas as pl
from jax.experimental.pallas import tpu as pltpu
from jax.sharding import PartitionSpec as P

MESH = pl.DeviceIdType.MESH
F32 = jnp.float32
BF16 = jnp.bfloat16
BLOCK = 8
FIRST_COT = 3
EARLY_IN = 1
LATE = 2
RELAY_AT = 5
EARLY_TURNS = 2
INPUT_GATE = 3


def swish(values):
    return values * jax.nn.sigmoid(values)


def swish_slope(values):
    logistic = jax.nn.sigmoid(values)
    return logistic * (1.0 + values * (1.0 - logistic))


def dot(left, right):
    return jnp.dot(left, right, preferred_element_type=F32)


def contract_last(left, right):
    return lax.dot_general(left, right, (((1,), (1,)), ((), ())), preferred_element_type=F32)


def chunk_of(width):
    return 256 if width % 256 == 0 else 128


def kernel(
    sizes,
    x_hbm, c_hbm, saved_hbm, ids_hbm, keep_hbm, slot_hbm, level_hbm,
    gate_r_hbm, up_r_hbm, down_r_hbm, gate_s_hbm, up_s_hbm, down_s_hbm,
    out_ref, grad_ref,
    gate_r, up_r, down_r, gate_s, up_s, down_s, down_peer,
    tables, tables_next, x_own, c_own, full_x, full_c, full_s,
    a_saved, b_saved, grad_hid, pre, pre_peer, late, late_w, hidden, grad_gate, grad_up,
    a_routed, b_routed,
    send_s, send_c, send_x, held_x, relay_x, recv_s, recv_c, recv_x, rows,
    back_send_g, back_recv_g, back_send_o, back_recv_o, back_rows,
    gate_rt, up_rt, down_rt, gate_st, up_st,
    part_grad, peer_grad, out_sum, factor_high, factor_low, factor_grad,
    weight_sem, table_sem, local_sem,
    next_send, next_recv, saved_send, saved_recv, down_send, down_recv,
    c_send, c_recv, x_send, x_recv, cf_send, cf_recv, xf_send, xf_recv,
    rs_send, rs_recv, rc_send, rc_recv, rx_send, rx_recv, pick_send, pick_recv,
    bg_send, bg_recv, bo_send, bo_recv, part_send, part_recv, pre_send, pre_recv,
    late_send, late_recv,
):
    n_pipe, ne, nt, capacity = sizes
    tokens, width = x_own.shape
    features = width * nt
    experts, blocks = send_s.shape[0], send_x.shape[0]
    folds = width // send_s.shape[2]
    me_p, me_e, me_t = lax.axis_index("pipe"), lax.axis_index("expert"), lax.axis_index("tensor")
    nxt, prv = lax.rem(me_p + 1, n_pipe), lax.rem(me_p + n_pipe - 1, n_pipe)
    my_cols = pl.ds(pl.multiple_of(me_t * width, 128), width)
    cw = chunk_of(width)
    chunks = width // cw
    last_p = n_pipe - 1

    def peer_t(step):
        return lax.rem(me_t + step, nt)

    def peer_e(step):
        return lax.rem(me_e + step, ne)

    def source_t(step):
        return lax.rem(me_t + nt - step, nt)

    def planned(src, dst, ssem, rsem, device):
        return pltpu.make_async_remote_copy(
            src_ref=src, dst_ref=dst, send_sem=ssem, recv_sem=rsem,
            device_id=device, device_id_type=MESH,
        )

    def remote(src, dst, ssem, rsem, device):
        copy = planned(src, dst, ssem, rsem, device)
        copy.start()
        return copy

    def sent(whole, sem):
        planned(whole, whole, sem, sem, {"pipe": nxt}).wait_send()

    def received(whole, sem):
        planned(whole, whole, sem, sem, {"pipe": nxt}).wait_recv()

    def load(src, dst, sem):
        copy = pltpu.make_async_copy(src, dst, sem)
        copy.start()
        return copy

    def local_cols(n):
        return pl.ds(n * cw, cw)

    def cols_of(part, n):
        return pl.ds(pl.multiple_of(part * width + n * cw, 128), cw)

    c_load = load(c_hbm, c_own, local_sem.at[0])
    for a, src in enumerate((ids_hbm, keep_hbm, slot_hbm, level_hbm)):
        load(src, tables.at[a], table_sem)
    saved_load = load(saved_hbm, full_s.at[:, my_cols], local_sem.at[1])
    x_load = load(x_hbm, x_own, local_sem.at[2])

    barrier = pltpu.get_barrier_semaphore()
    greeted = [{"pipe": nxt}, {"pipe": prv}]
    for se in range(ne):
        for st in range(nt):
            if se or st:
                greeted.append({"expert": peer_e(se), "tensor": peer_t(st)})
    for device in greeted:
        pl.semaphore_signal(barrier, inc=1, device_id=device, device_id_type=MESH)
    c_load.wait()
    gate_s_load = load(gate_s_hbm, gate_s, weight_sem.at[0])
    up_s_load = load(up_s_hbm, up_s, weight_sem.at[1])
    gate_r_load = load(gate_r_hbm, gate_r, weight_sem.at[2])
    up_r_load = load(up_r_hbm, up_r, weight_sem.at[3])
    down_s_load = load(down_s_hbm, down_s, weight_sem.at[4])
    down_r_load = load(down_r_hbm, down_r, weight_sem.at[5])
    pl.semaphore_wait(barrier, len(greeted))

    pltpu.make_async_copy(tables, tables, table_sem).wait()
    for a in range(3):
        remote(tables.at[a, 0], tables_next.at[a], next_send, next_recv, {"pipe": prv})
    c_copies = [
        planned(
            c_own.at[:, local_cols(n)], full_c.at[:, cols_of(me_t, n)],
            c_send, c_recv.at[n], {"pipe": prv},
        )
        for n in range(chunks)
    ]
    x_copies = [
        planned(
            x_own.at[:, local_cols(n)], full_x.at[:, cols_of(me_t, n)],
            x_send, x_recv.at[n], {"pipe": nxt},
        )
        for n in range(chunks)
    ]
    for n in range(FIRST_COT):
        c_copies[n].start()
    saved_load.wait()
    x_load.wait()
    saved_copies = [
        remote(
            full_s.at[:, my_cols], full_s.at[:, my_cols], saved_send.at[st - 1],
            saved_recv.at[st - 1], {"tensor": peer_t(st)},
        )
        for st in range(1, nt)
    ]
    down_copies = []
    for st in range(1, nt):
        to = peer_t(st)
        down_copies.append(remote(
            down_s_hbm.at[:, pl.ds(pl.multiple_of(to * width, 128), width)], down_peer.at[st - 1],
            down_send.at[st - 1], down_recv.at[st - 1], {"tensor": to},
        ))
        for part in range(nt):
            at = pl.ds(part * width + (chunks - LATE) * cw, LATE * cw)
            for a, src in enumerate((gate_s_hbm, up_s_hbm)):
                remote(
                    src.at[at, :], late_w.at[a, st - 1, part], late_send, late_recv, {"tensor": to}
                )

    def table(target, values, slots_at):
        total = jnp.zeros((slots_at.shape[0], tokens), jnp.int32)
        for k in range(target.shape[0]):
            total = total + jnp.where(target[k:k + 1] == slots_at, values[k:k + 1], 0)
        return total

    def targets(ids, keep, slot):
        return jnp.where(keep > 0, ids * capacity + slot, -1)

    target_f = targets(tables[0, 0], tables[1, 0], tables[2, 0])
    target_b = targets(tables[0, 1], tables[1, 1], tables[2, 1])
    level_f, level_b = tables[3, 0], tables[3, 1]
    used = max(16, blocks * BLOCK)
    place = lax.broadcasted_iota(jnp.int32, (used, tokens), 0)
    ones = jnp.ones(target_f.shape, jnp.int32)
    pick_b = table(target_b, ones, place).astype(F32).astype(BF16)
    scale_b = jnp.sum(table(target_b, level_b, place).astype(F32), axis=1, keepdims=True) / 4096.0

    def pack(values):
        half = width // folds
        return jnp.concatenate((values[:, :half], values[:, width - half:]), axis=0).astype(BF16)

    def unpack(values):
        held = values.astype(F32)
        pieces = [held[f * capacity:(f + 1) * capacity] for f in range(folds)]
        return jnp.concatenate(pieces, axis=1)

    def exchange(buffer, landing, ssem, rsem):
        for se in range(ne):
            for st in range(nt):
                if se or st:
                    to_e, n = peer_e(se), min(se, 1)
                    remote(
                        buffer.at[lax.div(to_e, 2)], landing.at[me_e, me_t], ssem.at[n], rsem.at[n],
                        {"expert": to_e, "tensor": peer_t(st)},
                    )
        landing[me_e, me_t] = buffer[lax.div(me_e, 2)]

    def near(landing):
        return landing.at[0, pl.ds(0, nt - 1)]

    def far(landing):
        return landing.at[pl.ds(0, ne - 1)]

    def wait_rows(landing, rsem):
        received(near(landing), rsem.at[0])
        received(far(landing), rsem.at[1])

    def wait_rows_sent(landing, ssem):
        sent(near(landing), ssem.at[0])
        sent(far(landing), ssem.at[1])

    group = 16 // capacity

    def gather_rows(landing):
        for t in range(nt):
            for i in range(0, ne, group):
                held = [unpack(landing[j, t]) for j in range(i, i + group)]
                rows[i * capacity:(i + group) * capacity, t * width:(t + 1) * width] = (
                    jnp.concatenate(held, axis=0).astype(BF16)
                )

    def pick_rows(picks, read):
        return jnp.concatenate([dot(picks, read(n)) for n in range(chunks)], axis=1)

    def fill(buffer, picked):
        for k in range(experts):
            buffer[k] = pack(picked[k * capacity:(k + 1) * capacity])

    fill(send_s, pick_rows(pick_b, lambda n: full_s[:, cols_of(me_t, n)]))
    exchange(send_s, recv_s, rs_send, rs_recv)

    parts = ne * nt * capacity
    place_b = lax.broadcasted_iota(jnp.int32, (parts, tokens), 0)
    expert = lax.div(lax.div(place_b, nt * capacity), 2)
    slots = expert * capacity + lax.rem(place_b, capacity)
    level = table(target_f, level_f, slots)
    high = lax.div(level, 64)
    low = level - high * 64
    factor_high[...] = (high.astype(F32) / 64.0).T.astype(BF16)
    factor_low[...] = (low.astype(F32) / 4096.0).T.astype(BF16)
    factor_grad[...] = table(target_b, ones, slots).astype(F32).T.astype(BF16)

    for copy in saved_copies:
        copy.wait_recv()
    gate_s_load.wait()
    up_s_load.wait()
    cs = chunk_of(gate_s.shape[1])

    for n in range(gate_s.shape[1] // cs):
        cols = pl.ds(n * cs, cs)
        gate_back = dot(full_s[...], gate_s[:, cols])
        up_back = dot(full_s[...], up_s[:, cols])
        a_saved[:, cols] = up_back * swish_slope(gate_back)
        b_saved[:, cols] = swish(gate_back)

    received(tables_next, next_recv)
    target_n = targets(tables_next[0], tables_next[1], tables_next[2])
    pick_n = table(target_n, ones, place).astype(F32).astype(BF16)

    picked = pick_rows(pick_n, lambda n: x_own[:, local_cols(n)])
    for b in range(blocks):
        send_x[b] = picked[b * BLOCK:(b + 1) * BLOCK].astype(BF16)
    picked_copy = remote(send_x, held_x, pick_send, pick_recv, {"pipe": nxt})

    order = [(c_copies, n) for n in range(FIRST_COT, chunks)]
    early = list(order)
    for m in range(EARLY_IN):
        early.insert(len(early) - 2 * EARLY_IN + 1 + 2 * m, (x_copies, m))

    @pl.when(me_p == last_p)
    def _():
        for kind, n in early:
            kind[n].start()

    @pl.when(me_p != last_p)
    def _():
        for kind, n in order:
            kind[n].start()

    for load_done in (gate_r_load, up_r_load, down_r_load):
        load_done.wait()
    turned = features // chunks

    def turn(n):
        at = pl.ds(n * turned, turned)
        gate_st[:, at] = gate_s[at, :].T
        up_st[:, at] = up_s[at, :].T
        gate_rt[:, at] = gate_r[at, :].T
        up_rt[:, at] = up_r[at, :].T
        down_rt[at, :] = down_r[:, at].T

    for n in range(EARLY_TURNS):
        turn(n)

    wait_rows(recv_s, rs_recv)
    gather_rows(recv_s)
    gate_back = dot(rows[...], gate_r[...])
    a_routed[...] = dot(rows[...], up_r[...]) * swish_slope(gate_back)
    b_routed[...] = swish(gate_back)

    down_s_load.wait()

    def forward(held, n, ssem, rsem):
        cols = cols_of(me_t, n)
        return [
            remote(
                held.at[:, cols], held.at[:, cols], ssem.at[st - 1], rsem.at[n, st - 1],
                {"tensor": peer_t(st)},
            )
            for st in range(1, nt)
        ]

    def add_cot(part, n, first=False):
        cols = cols_of(part, n)
        piece = contract_last(full_c[:, cols], down_s[:, cols])
        grad_hid[...] = piece if first else grad_hid[...] + piece

    def add_forwarded(copies, n, add):
        for st in range(1, nt):
            copies[st - 1].wait_recv()
            add(source_t(st), n)

    cf_copies = []
    for n in range(chunks):
        c_copies[n].wait_recv()
        cf_copies.append(forward(full_c, n, cf_send, cf_recv))
        if n == INPUT_GATE:
            @pl.when(me_p != last_p)
            def _():
                for m in range(EARLY_IN):
                    x_copies[m].start()

            for m in range(EARLY_IN, chunks):
                x_copies[m].start()
        if n == chunks - 1:
            fill(send_c, scale_b * pick_rows(pick_b, lambda m: full_c[:, cols_of(me_t, m)]))
            exchange(send_c, recv_c, rc_send, rc_recv)
        if n == RELAY_AT:
            picked_copy.wait_recv()
            for k in range(experts):
                b, at = divmod(k * capacity, BLOCK)
                relay_x[k] = pack(held_x[b].astype(F32)[at:at + capacity])
            exchange(relay_x, recv_x, rx_send, rx_recv)
        add_cot(me_t, n, first=n == 0)
        if n + EARLY_TURNS < chunks:
            turn(n + EARLY_TURNS)
        if n:
            add_forwarded(cf_copies[n - 1], n - 1, add_cot)
    xf_copies = []

    def land_in(n):
        x_copies[n].wait_recv()
        xf_copies.append(forward(full_x, n, xf_send, xf_recv))

    def send_back(total_of, buffer, landing, ssem, rsem):
        for st in list(range(1, nt)) + [0]:
            to_t = peer_t(st)
            total = jnp.concatenate([total_of(cols_of(to_t, n)) for n in range(chunks)], axis=1)
            for i in range(ne):
                buffer[i, to_t] = pack(total[i * capacity:(i + 1) * capacity])
            for se in range(ne):
                if se or st:
                    to_e, n = peer_e(se), min(se, 1)
                    remote(
                        buffer.at[to_e, to_t], landing.at[me_e, me_t], ssem.at[n], rsem.at[n],
                        {"expert": to_e, "tensor": to_t},
                    )
        landing[me_e, me_t] = buffer[me_e, me_t]

    add_forwarded(cf_copies[chunks - 1], chunks - 1, add_cot)
    grad_gate[...] = (grad_hid[...] * a_saved[...]).astype(BF16)
    grad_up[...] = (grad_hid[...] * b_saved[...]).astype(BF16)
    part_copies = []
    for st in list(range(1, nt)) + [0]:
        to = peer_t(st)
        for n in range(chunks):
            cols = cols_of(to, n)
            part_grad[st, :, local_cols(n)] = (
                dot(grad_gate[...], gate_st[:, cols]) + dot(grad_up[...], up_st[:, cols])
            )
        if st:
            part_copies.append(remote(
                part_grad.at[st], peer_grad.at[st - 1], part_send.at[st - 1],
                part_recv.at[st - 1], {"tensor": to},
            ))
    land_in(0)

    wait_rows(recv_x, rx_recv)
    gather_rows(recv_x)
    gate_fwd = dot(rows[...], gate_r[...])
    hidden_r = (swish(gate_fwd) * dot(rows[...], up_r[...])).astype(BF16)
    send_back(
        lambda cols: dot(hidden_r, down_r[:, cols]), back_send_o, back_recv_o, bo_send, bo_recv
    )
    wait_rows(recv_c, rc_recv)
    gather_rows(recv_c)
    grad_back = dot(rows[...], down_rt[...])
    gate_grad_r = (grad_back * a_routed[...]).astype(BF16)
    up_grad_r = (grad_back * b_routed[...]).astype(BF16)
    send_back(
        lambda cols: dot(gate_grad_r, gate_rt[:, cols]) + dot(up_grad_r, up_rt[:, cols]),
        back_send_g, back_recv_g, bg_send, bg_recv,
    )
    land_in(1)

    land_in(2)

    def gather_back(landing):
        for i in range(0, ne * nt, group):
            held = [unpack(landing[divmod(j, nt)]) for j in range(i, i + group)]
            back_rows[i * capacity:(i + group) * capacity, :] = (
                jnp.concatenate(held, axis=0).astype(BF16)
            )

    def finish_grad():
        wait_rows(back_recv_g, bg_recv)
        gather_back(back_recv_g)
        for copy in part_copies:
            copy.wait_recv()

        for n in range(chunks):
            at = local_cols(n)
            total = part_grad[0, :, at] + dot(factor_grad[...], back_rows[:, at])
            for st in range(1, nt):
                total = total + peer_grad[st - 1, :, at]
            grad_ref[:, at] = total.astype(BF16)

    early_n = chunks - LATE

    def arrived(n):
        for copy in xf_copies[n]:
            copy.wait_recv()

    def add_in(spans, first=False):
        for a, weight in enumerate((gate_s, up_s)):
            piece = 0.0
            for part, n in spans:
                cols = cols_of(part, n)
                piece = piece + dot(full_x[:, cols], weight[cols, :])
            pre[a] = piece if first else pre[a] + piece

    for n in range(3, early_n - 1):
        land_in(n)
    for n in range(early_n - 1):
        arrived(n)
    add_in([(source_t(st), n) for n in range(early_n - 1) for st in range(nt)], first=True)
    land_in(early_n - 1)
    land_in(early_n)
    add_in([(me_t, early_n - 1)])
    arrived(early_n - 1)
    add_in([(source_t(st), early_n - 1) for st in range(1, nt)])

    pre_copies = [
        remote(
            pre, pre_peer.at[st - 1], pre_send.at[st - 1], pre_recv.at[st - 1],
            {"tensor": peer_t(st)},
        )
        for st in range(1, nt)
    ]
    wait_rows(back_recv_o, bo_recv)
    gather_back(back_recv_o)
    for n in range(chunks):
        at = local_cols(n)
        held = back_rows[:, at]
        out_sum[:, at] = dot(factor_high[...], held) + dot(factor_low[...], held)
    finish_grad()
    for copy in down_copies:
        copy.wait_recv()
    received(late_w, late_recv)
    sent(c_own, c_send)
    sent(tables_next, next_send)
    sent(send_x, pick_send)
    for landing, sem in (
        (recv_s, rs_send), (recv_c, rc_send), (recv_x, rx_send),
        (back_recv_g, bg_send), (back_recv_o, bo_send),
    ):
        wait_rows_sent(landing, sem)
    sent(late_w, late_send)
    for copy in saved_copies + down_copies + part_copies:
        copy.wait_send()
    for st in range(1, nt):
        sent(full_c.at[:, my_cols], cf_send.at[st - 1])
    def late_piece(unit, a, part, n):
        cols = cols_of(part, n)
        if unit:
            at = (n - early_n) * cw
            return dot(full_x[:, cols], late_w[a, unit - 1, part, at:at + cw, :])
        return dot(full_x[:, cols], (gate_s, up_s)[a][cols, :])

    for n in range(early_n, chunks - 1):
        arrived(n)
    for unit in range(nt):
        for a in range(2):
            total = pre[a] if unit == 0 else 0.0
            for n in range(early_n, chunks - 1):
                for st in range(nt):
                    total = total + late_piece(unit, a, source_t(st), n)
            late[unit, a] = total
    land_in(chunks - 1)
    for unit in range(nt):
        for a in range(2):
            late[unit, a] = late[unit, a] + late_piece(unit, a, me_t, chunks - 1)
    for copy in pre_copies:
        copy.wait_recv()
    arrived(chunks - 1)
    for unit in range(nt):
        total = [late[unit, 0], late[unit, 1]]
        for a in range(2):
            if unit:
                total[a] = total[a] + pre_peer[unit - 1, a]
            for st in range(1, nt):
                total[a] = total[a] + late_piece(unit, a, source_t(st), chunks - 1)
        hidden[unit] = (swish(total[0]) * total[1]).astype(BF16)
    for n in range(chunks):
        at = local_cols(n)
        total = out_sum[:, at] + dot(hidden[0], down_s[:, cols_of(me_t, n)])
        for st in range(1, nt):
            total = total + dot(hidden[st], down_peer[st - 1, :, at])
        out_ref[:, at] = total.astype(BF16)

    sent(x_own, x_send)
    for st in range(1, nt):
        sent(full_x.at[:, my_cols], xf_send.at[st - 1])
    for copy in pre_copies:
        copy.wait_send()


def store(out, grad, out_hbm, grad_hbm, sem):
    first = pltpu.make_async_copy(out, out_hbm, sem.at[0])
    second = pltpu.make_async_copy(grad, grad_hbm, sem.at[1])
    first.start()
    second.start()
    first.wait()
    second.wait()


def lanes_last(choices):
    return jnp.swapaxes(choices[:, 0], 1, 2)


def in_hbm(values):
    return pltpu.with_memory_space_constraint(values, pltpu.HBM)


def local(
    inputs_prev, cotangent_next, saved_input, expert_ids, keep_mask, slot_pos, weight_q,
    gate_routed, up_routed, down_routed, gate_shared, up_shared, down_shared,
):
    n_pipe, ne, nt = lax.axis_size("pipe"), lax.axis_size("expert"), lax.axis_size("tensor")
    tokens, width = inputs_prev.shape[1:]
    topk = expert_ids.shape[3]
    features = width * nt
    capacity = tokens // 32
    experts = ne // 2
    blocks = -(-experts * capacity // BLOCK)
    folded = width // 2 if width % 256 == 0 else width
    fr, fs = gate_routed.shape[3], gate_shared.shape[2]
    chunks = width // chunk_of(width)
    peers = ne * nt - 1
    vmem = pl.BlockSpec(memory_space=pltpu.VMEM)
    hbm = pl.BlockSpec(memory_space=pl.ANY)
    dma = pltpu.SemaphoreType.DMA
    shape = pltpu.VMEM((tokens, width), BF16)
    out, grad = pl.pallas_call(
        functools.partial(kernel, (n_pipe, ne, nt, capacity)),
        out_shape=(shape, shape),
        in_specs=[hbm] * 13,
        out_specs=(vmem, vmem),
        scratch_shapes=[
            pltpu.VMEM((features, fr), BF16),
            pltpu.VMEM((features, fr), BF16),
            pltpu.VMEM((fr, features), BF16),
            pltpu.VMEM((features, fs), BF16),
            pltpu.VMEM((features, fs), BF16),
            pltpu.VMEM((fs, features), BF16),
            pltpu.VMEM((nt - 1, fs, width), BF16),
            pltpu.VMEM((4, 2, topk, tokens), jnp.int32),
            pltpu.VMEM((3, topk, tokens), jnp.int32),
            pltpu.VMEM((tokens, width), BF16),
            pltpu.VMEM((tokens, width), BF16),
            pltpu.VMEM((tokens, features), BF16),
            pltpu.VMEM((tokens, features), BF16),
            pltpu.VMEM((tokens, features), BF16),
            pltpu.VMEM((tokens, fs), F32),
            pltpu.VMEM((tokens, fs), F32),
            pltpu.VMEM((tokens, fs), F32),
            pltpu.VMEM((2, tokens, fs), F32),
            pltpu.VMEM((nt - 1, 2, tokens, fs), F32),
            pltpu.VMEM((nt, 2, tokens, fs), F32),
            pltpu.VMEM((2, nt - 1, nt, LATE * chunk_of(width), fs), BF16),
            pltpu.VMEM((nt, tokens, fs), BF16),
            pltpu.VMEM((tokens, fs), BF16),
            pltpu.VMEM((tokens, fs), BF16),
            pltpu.VMEM((ne * capacity, fr), F32),
            pltpu.VMEM((ne * capacity, fr), F32),
            pltpu.VMEM((experts, BLOCK, folded), BF16),
            pltpu.VMEM((experts, BLOCK, folded), BF16),
            pltpu.VMEM((blocks, BLOCK, width), BF16),
            pltpu.VMEM((blocks, BLOCK, width), BF16),
            pltpu.VMEM((experts, BLOCK, folded), BF16),
            pltpu.VMEM((ne, nt, BLOCK, folded), BF16),
            pltpu.VMEM((ne, nt, BLOCK, folded), BF16),
            pltpu.VMEM((ne, nt, BLOCK, folded), BF16),
            pltpu.VMEM((ne * capacity, features), BF16),
            pltpu.VMEM((ne, nt, BLOCK, folded), BF16),
            pltpu.VMEM((ne, nt, BLOCK, folded), BF16),
            pltpu.VMEM((ne, nt, BLOCK, folded), BF16),
            pltpu.VMEM((ne, nt, BLOCK, folded), BF16),
            pltpu.VMEM((ne * nt * capacity, width), BF16),
            pltpu.VMEM((fr, features), BF16),
            pltpu.VMEM((fr, features), BF16),
            pltpu.VMEM((features, fr), BF16),
            pltpu.VMEM((fs, features), BF16),
            pltpu.VMEM((fs, features), BF16),
            pltpu.VMEM((nt, tokens, width), F32),
            pltpu.VMEM((nt - 1, tokens, width), F32),
            pltpu.VMEM((tokens, width), F32),
            pltpu.VMEM((tokens, ne * nt * capacity), BF16),
            pltpu.VMEM((tokens, ne * nt * capacity), BF16),
            pltpu.VMEM((tokens, ne * nt * capacity), BF16),
            dma((6,)), dma, dma((3,)),
            dma, dma,
            dma((nt - 1,)), dma((nt - 1,)), dma((nt - 1,)), dma((nt - 1,)),
            dma, dma((chunks,)), dma, dma((chunks,)),
            dma((nt - 1,)), dma((chunks, nt - 1)),
            dma((nt - 1,)), dma((chunks, nt - 1)),
            dma((2,)), dma((2,)), dma((2,)), dma((2,)),
            dma((2,)), dma((2,)), dma, dma,
            dma((2,)), dma((2,)), dma((2,)), dma((2,)),
            dma((nt - 1,)), dma((nt - 1,)), dma((nt - 1,)), dma((nt - 1,)),
            dma, dma,
        ],
        compiler_params=pltpu.CompilerParams(
            collective_id=0, has_side_effects=True, vmem_limit_bytes=60 * 1024 * 1024
        ),
        name="moe_step",
    )(
        *(in_hbm(v) for v in (
            inputs_prev[0], cotangent_next[0], saved_input[0],
            *(lanes_last(v) for v in (expert_ids, keep_mask, slot_pos, weight_q)),
            gate_routed[0, 0], up_routed[0, 0], down_routed[0, 0],
            gate_shared[0], up_shared[0], down_shared[0],
        ))
    )
    result = jax.ShapeDtypeStruct((tokens, width), BF16)
    out, grad = pl.pallas_call(
        store,
        out_shape=(result, result),
        in_specs=[vmem] * 2,
        out_specs=(hbm, hbm),
        scratch_shapes=[dma((2,))],
        compiler_params=pltpu.CompilerParams(vmem_limit_bytes=2 * 1024 * 1024),
        name="store_out",
    )(*(pltpu.with_memory_space_constraint(v, pltpu.VMEM) for v in (out, grad)))
    return out[None], grad[None]


def solution(mesh):
    return jax.shard_map(
        local,
        mesh=mesh,
        in_specs=(
            P("pipe", "expert", "tensor"),
            P("pipe", "expert", "tensor"),
            P("pipe", "expert", "tensor"),
            P(None, "pipe", "expert", None),
            P(None, "pipe", "expert", None),
            P(None, "pipe", "expert", None),
            P(None, "pipe", "expert", None),
            P("pipe", "expert", None, "tensor"),
            P("pipe", "expert", None, "tensor"),
            P("pipe", "expert", "tensor", None),
            P("pipe", None, "tensor"),
            P("pipe", None, "tensor"),
            P("pipe", "tensor", None),
        ),
        out_specs=(P("pipe", "expert", "tensor"), P("pipe", "expert", "tensor")),
        check_vma=False,
    )
```

```python
import functools

import jax
import jax.numpy as jnp
from jax import lax
from jax.experimental import pallas as pl
from jax.experimental.pallas import tpu as pltpu
from jax.sharding import PartitionSpec as P

MESH = pl.DeviceIdType.MESH
F32 = jnp.float32
BF16 = jnp.bfloat16
BLOCK = 8
FIRST_COT = 3
EARLY_IN = 1
LATE = 2
RELAY_AT = 5
EARLY_TURNS = 2
INPUT_GATE = 3


def swish(values):
    return values * jax.nn.sigmoid(values)


def swish_slope(values):
    logistic = jax.nn.sigmoid(values)
    return logistic * (1.0 + values * (1.0 - logistic))


def dot(left, right):
    return jnp.dot(left, right, preferred_element_type=F32)


def contract_last(left, right):
    return lax.dot_general(left, right, (((1,), (1,)), ((), ())), preferred_element_type=F32)


def chunk_of(width):
    return 256 if width % 256 == 0 else 128


def kernel(
    sizes,
    x_hbm, c_hbm, saved_hbm, ids_hbm, keep_hbm, slot_hbm, level_hbm,
    gate_r_hbm, up_r_hbm, down_r_hbm, gate_s_hbm, up_s_hbm, down_s_hbm,
    out_ref, grad_ref,
    gate_r, up_r, down_r, gate_s, up_s, down_s, down_peer,
    tables, tables_next, x_own, c_own, full_x, full_c, full_s,
    a_saved, b_saved, grad_hid, pre, pre_peer, late, late_w, hidden, drain, grad_gate, grad_up,
    a_routed, b_routed,
    send_s, send_c, send_x, held_x, relay_x, recv_s, recv_c, recv_x, rows,
    back_send_g, back_recv_g, back_send_o, back_recv_o, back_rows,
    gate_rt, up_rt, down_rt, gate_st, up_st,
    part_grad, peer_grad, out_sum, factor_high, factor_low, factor_grad,
    weight_sem, table_sem, local_sem, send_sem, entry_sem,
    next_recv, saved_recv, down_recv, c_recv, x_recv, cf_recv, xf_recv,
    rs_recv, rc_recv, rx_recv, pick_recv, bg_recv, bo_recv, part_recv, pre_recv, late_recv,
):
    n_pipe, ne, nt, capacity = sizes
    tokens, width = x_own.shape
    features = width * nt
    experts, blocks = send_s.shape[0], send_x.shape[0]
    folds = width // send_s.shape[2]
    peers = ne * nt - 1
    row_lines = BLOCK * send_s.shape[2] // 128
    me_p, me_e, me_t = lax.axis_index("pipe"), lax.axis_index("expert"), lax.axis_index("tensor")
    nxt, prv = lax.rem(me_p + 1, n_pipe), lax.rem(me_p + n_pipe - 1, n_pipe)
    my_cols = pl.ds(pl.multiple_of(me_t * width, 128), width)
    cw = chunk_of(width)
    chunks = width // cw
    last_p = n_pipe - 1

    def peer_t(step):
        return lax.rem(me_t + step, nt)

    def peer_e(step):
        return lax.rem(me_e + step, ne)

    def source_t(step):
        return lax.rem(me_t + nt - step, nt)

    def planned(src, dst, ssem, rsem, device):
        return pltpu.make_async_remote_copy(
            src_ref=src, dst_ref=dst, send_sem=ssem, recv_sem=rsem,
            device_id=device, device_id_type=MESH,
        )

    def remote(src, dst, ssem, rsem, device):
        copy = planned(src, dst, ssem, rsem, device)
        copy.start()
        return copy

    def received(whole, sem):
        planned(whole, whole, sem, sem, {"pipe": nxt}).wait_recv()

    def load(src, dst, sem):
        copy = pltpu.make_async_copy(src, dst, sem)
        copy.start()
        return copy

    def local_cols(n):
        return pl.ds(n * cw, cw)

    def cols_of(part, n):
        return pl.ds(pl.multiple_of(part * width + n * cw, 128), cw)

    c_load = load(c_hbm, c_own, local_sem.at[0])
    for a, src in enumerate((ids_hbm, keep_hbm, slot_hbm, level_hbm)):
        load(src, tables.at[a], table_sem)
    saved_load = load(saved_hbm, full_s.at[:, my_cols], local_sem.at[1])
    x_load = load(x_hbm, x_own, local_sem.at[2])

    barrier = pltpu.get_barrier_semaphore()
    mate = me_e + 1 - 2 * lax.rem(me_e, 2)
    greeted = [{"pipe": nxt}, {"pipe": prv}]
    for st in range(nt):
        greeted.append({"expert": mate, "tensor": peer_t(st)})
        for se in range(0, ne, 2):
            if se or st:
                greeted.append({"expert": peer_e(se), "tensor": peer_t(st)})
    for device in greeted:
        pl.semaphore_signal(barrier, inc=1, device_id=device, device_id_type=MESH)
    c_load.wait()
    gate_s_load = load(gate_s_hbm, gate_s, weight_sem.at[0])
    up_s_load = load(up_s_hbm, up_s, weight_sem.at[1])
    gate_r_load = load(gate_r_hbm, gate_r, weight_sem.at[2])
    up_r_load = load(up_r_hbm, up_r, weight_sem.at[3])
    down_s_load = load(down_s_hbm, down_s, weight_sem.at[4])
    down_r_load = load(down_r_hbm, down_r, weight_sem.at[5])
    pl.semaphore_wait(barrier, len(greeted))
    pl.semaphore_signal(entry_sem, inc=1, device_id={"expert": mate}, device_id_type=MESH)

    pltpu.make_async_copy(tables, tables, table_sem).wait()
    for a in range(3):
        remote(tables.at[a, 0], tables_next.at[a], send_sem, next_recv, {"pipe": prv})
    c_copies = [
        planned(
            c_own.at[:, local_cols(n)], full_c.at[:, cols_of(me_t, n)],
            send_sem, c_recv.at[n], {"pipe": prv},
        )
        for n in range(chunks)
    ]
    x_copies = [
        planned(
            x_own.at[:, local_cols(n)], full_x.at[:, cols_of(me_t, n)],
            send_sem, x_recv.at[n], {"pipe": nxt},
        )
        for n in range(chunks)
    ]
    for n in range(FIRST_COT):
        c_copies[n].start()
    saved_load.wait()
    x_load.wait()
    saved_copies = [
        remote(
            full_s.at[:, my_cols], full_s.at[:, my_cols], send_sem,
            saved_recv.at[st - 1], {"tensor": peer_t(st)},
        )
        for st in range(1, nt)
    ]
    down_copies = []
    for st in range(1, nt):
        to = peer_t(st)
        down_copies.append(remote(
            down_s_hbm.at[:, pl.ds(pl.multiple_of(to * width, 128), width)], down_peer.at[st - 1],
            send_sem, down_recv.at[st - 1], {"tensor": to},
        ))
        for part in range(nt):
            at = pl.ds(part * width + (chunks - LATE) * cw, LATE * cw)
            for a, src in enumerate((gate_s_hbm, up_s_hbm)):
                remote(
                    src.at[at, :], late_w.at[a, st - 1, part], send_sem, late_recv, {"tensor": to}
                )

    def table(target, values, slots_at):
        total = jnp.zeros((slots_at.shape[0], tokens), jnp.int32)
        for k in range(target.shape[0]):
            total = total + jnp.where(target[k:k + 1] == slots_at, values[k:k + 1], 0)
        return total

    def targets(ids, keep, slot):
        return jnp.where(keep > 0, ids * capacity + slot, -1)

    target_f = targets(tables[0, 0], tables[1, 0], tables[2, 0])
    target_b = targets(tables[0, 1], tables[1, 1], tables[2, 1])
    level_f, level_b = tables[3, 0], tables[3, 1]
    used = max(16, blocks * BLOCK)
    place = lax.broadcasted_iota(jnp.int32, (used, tokens), 0)
    ones = jnp.ones(target_f.shape, jnp.int32)
    pick_b = table(target_b, ones, place).astype(F32).astype(BF16)
    scale_b = jnp.sum(table(target_b, level_b, place).astype(F32), axis=1, keepdims=True) / 4096.0

    def pack(values):
        half = width // folds
        return jnp.concatenate((values[:, :half], values[:, width - half:]), axis=0).astype(BF16)

    def unpack(values):
        held = values.astype(F32)
        pieces = [held[f * capacity:(f + 1) * capacity] for f in range(folds)]
        return jnp.concatenate(pieces, axis=1)

    def exchange(buffer, landing, rsem):
        for se in range(ne):
            for st in range(nt):
                if se or st:
                    to_e = peer_e(se)
                    remote(
                        buffer.at[lax.div(to_e, 2)], landing.at[me_e, me_t], send_sem, rsem,
                        {"expert": to_e, "tensor": peer_t(st)},
                    )
        landing[me_e, me_t] = buffer[lax.div(me_e, 2)]

    def wait_rows(rsem):
        received(drain.at[pl.ds(0, peers * row_lines)], rsem)

    group = 16 // capacity

    def gather_rows(landing):
        for t in range(nt):
            for i in range(0, ne, group):
                held = [unpack(landing[j, t]) for j in range(i, i + group)]
                rows[i * capacity:(i + group) * capacity, t * width:(t + 1) * width] = (
                    jnp.concatenate(held, axis=0).astype(BF16)
                )

    def pick_rows(picks, read):
        return jnp.concatenate([dot(picks, read(n)) for n in range(chunks)], axis=1)

    def fill(buffer, picked):
        for k in range(experts):
            buffer[k] = pack(picked[k * capacity:(k + 1) * capacity])

    fill(send_s, pick_rows(pick_b, lambda n: full_s[:, cols_of(me_t, n)]))
    pl.semaphore_wait(entry_sem, 1)
    exchange(send_s, recv_s, rs_recv)

    parts = ne * nt * capacity
    place_b = lax.broadcasted_iota(jnp.int32, (parts, tokens), 0)
    expert = lax.div(lax.div(place_b, nt * capacity), 2)
    slots = expert * capacity + lax.rem(place_b, capacity)
    level = table(target_f, level_f, slots)
    high = lax.div(level, 64)
    low = level - high * 64
    factor_high[...] = (high.astype(F32) / 64.0).T.astype(BF16)
    factor_low[...] = (low.astype(F32) / 4096.0).T.astype(BF16)
    factor_grad[...] = table(target_b, ones, slots).astype(F32).T.astype(BF16)

    for copy in saved_copies:
        copy.wait_recv()
    gate_s_load.wait()
    up_s_load.wait()
    cs = chunk_of(gate_s.shape[1])

    for n in range(gate_s.shape[1] // cs):
        cols = pl.ds(n * cs, cs)
        gate_back = dot(full_s[...], gate_s[:, cols])
        up_back = dot(full_s[...], up_s[:, cols])
        a_saved[:, cols] = up_back * swish_slope(gate_back)
        b_saved[:, cols] = swish(gate_back)

    received(tables_next, next_recv)
    target_n = targets(tables_next[0], tables_next[1], tables_next[2])
    pick_n = table(target_n, ones, place).astype(F32).astype(BF16)

    picked = pick_rows(pick_n, lambda n: x_own[:, local_cols(n)])
    for b in range(blocks):
        send_x[b] = picked[b * BLOCK:(b + 1) * BLOCK].astype(BF16)
    picked_copy = remote(send_x, held_x, send_sem, pick_recv, {"pipe": nxt})

    order = [(c_copies, n) for n in range(FIRST_COT, chunks)]
    early = list(order)
    for m in range(EARLY_IN):
        early.insert(len(early) - 2 * EARLY_IN + 1 + 2 * m, (x_copies, m))

    @pl.when(me_p == last_p)
    def _():
        for kind, n in early:
            kind[n].start()

    @pl.when(me_p != last_p)
    def _():
        for kind, n in order:
            kind[n].start()

    for load_done in (gate_r_load, up_r_load, down_r_load):
        load_done.wait()
    turned = features // chunks

    def turn(n):
        at = pl.ds(n * turned, turned)
        gate_st[:, at] = gate_s[at, :].T
        up_st[:, at] = up_s[at, :].T
        gate_rt[:, at] = gate_r[at, :].T
        up_rt[:, at] = up_r[at, :].T
        down_rt[at, :] = down_r[:, at].T

    for n in range(EARLY_TURNS):
        turn(n)

    wait_rows(rs_recv)
    gather_rows(recv_s)
    gate_back = dot(rows[...], gate_r[...])
    a_routed[...] = dot(rows[...], up_r[...]) * swish_slope(gate_back)
    b_routed[...] = swish(gate_back)

    down_s_load.wait()

    def forwards(held, n, rsem):
        cols = cols_of(me_t, n)
        return [
            planned(
                held.at[:, cols], held.at[:, cols], send_sem, rsem.at[n, st - 1],
                {"tensor": peer_t(st)},
            )
            for st in range(1, nt)
        ]

    def forward(held, n, rsem):
        copies = forwards(held, n, rsem)
        for copy in copies:
            copy.start()
        return copies

    def add_cot(part, n, first=False):
        cols = cols_of(part, n)
        piece = contract_last(full_c[:, cols], down_s[:, cols])
        grad_hid[...] = piece if first else grad_hid[...] + piece

    def add_forwarded(copies, n, add):
        for st in range(1, nt):
            copies[st - 1].wait_recv()
            add(source_t(st), n)

    cf_copies = []
    for n in range(chunks):
        c_copies[n].wait_recv()
        cf_copies.append(forward(full_c, n, cf_recv))
        if n == INPUT_GATE:
            @pl.when(me_p != last_p)
            def _():
                for m in range(EARLY_IN):
                    x_copies[m].start()

            for m in range(EARLY_IN, chunks):
                x_copies[m].start()
        if n == chunks - 1:
            fill(send_c, scale_b * pick_rows(pick_b, lambda m: full_c[:, cols_of(me_t, m)]))
            exchange(send_c, recv_c, rc_recv)
        if n == RELAY_AT:
            picked_copy.wait_recv()
            for k in range(experts):
                b, at = divmod(k * capacity, BLOCK)
                relay_x[k] = pack(held_x[b].astype(F32)[at:at + capacity])
            exchange(relay_x, recv_x, rx_recv)
        add_cot(me_t, n, first=n == 0)
        if n + EARLY_TURNS < chunks:
            turn(n + EARLY_TURNS)
        if n:
            add_forwarded(cf_copies[n - 1], n - 1, add_cot)
    xf_copies = []

    def land_in(n):
        x_copies[n].wait_recv()
        xf_copies.append(forward(full_x, n, xf_recv))

    def send_back(total_of, buffer, landing, rsem):
        for st in list(range(1, nt)) + [0]:
            to_t = peer_t(st)
            total = jnp.concatenate([total_of(cols_of(to_t, n)) for n in range(chunks)], axis=1)
            for i in range(ne):
                buffer[i, to_t] = pack(total[i * capacity:(i + 1) * capacity])
            for se in range(ne):
                if se or st:
                    to_e = peer_e(se)
                    remote(
                        buffer.at[to_e, to_t], landing.at[me_e, me_t], send_sem, rsem,
                        {"expert": to_e, "tensor": to_t},
                    )
        landing[me_e, me_t] = buffer[me_e, me_t]

    add_forwarded(cf_copies[chunks - 1], chunks - 1, add_cot)
    grad_gate[...] = (grad_hid[...] * a_saved[...]).astype(BF16)
    grad_up[...] = (grad_hid[...] * b_saved[...]).astype(BF16)
    part_copies = []
    for st in list(range(1, nt)) + [0]:
        to = peer_t(st)
        for n in range(chunks):
            cols = cols_of(to, n)
            part_grad[st, :, local_cols(n)] = (
                dot(grad_gate[...], gate_st[:, cols]) + dot(grad_up[...], up_st[:, cols])
            )
        if st:
            part_copies.append(remote(
                part_grad.at[st], peer_grad.at[st - 1], send_sem,
                part_recv.at[st - 1], {"tensor": to},
            ))
    land_in(0)

    wait_rows(rx_recv)
    gather_rows(recv_x)
    gate_fwd = dot(rows[...], gate_r[...])
    hidden_r = (swish(gate_fwd) * dot(rows[...], up_r[...])).astype(BF16)
    send_back(
        lambda cols: dot(hidden_r, down_r[:, cols]), back_send_o, back_recv_o, bo_recv
    )
    wait_rows(rc_recv)
    gather_rows(recv_c)
    grad_back = dot(rows[...], down_rt[...])
    gate_grad_r = (grad_back * a_routed[...]).astype(BF16)
    up_grad_r = (grad_back * b_routed[...]).astype(BF16)
    send_back(
        lambda cols: dot(gate_grad_r, gate_rt[:, cols]) + dot(up_grad_r, up_rt[:, cols]),
        back_send_g, back_recv_g, bg_recv,
    )
    land_in(1)

    land_in(2)

    def gather_back(landing):
        for i in range(0, ne * nt, group):
            held = [unpack(landing[divmod(j, nt)]) for j in range(i, i + group)]
            back_rows[i * capacity:(i + group) * capacity, :] = (
                jnp.concatenate(held, axis=0).astype(BF16)
            )

    def finish_grad():
        wait_rows(bg_recv)
        gather_back(back_recv_g)
        for copy in part_copies:
            copy.wait_recv()

        for n in range(chunks):
            at = local_cols(n)
            total = part_grad[0, :, at] + dot(factor_grad[...], back_rows[:, at])
            for st in range(1, nt):
                total = total + peer_grad[st - 1, :, at]
            grad_ref[:, at] = total.astype(BF16)

    early_n = chunks - LATE

    def arrived(n):
        for copy in xf_copies[n]:
            copy.wait_recv()

    def add_in(spans, first=False):
        for a, weight in enumerate((gate_s, up_s)):
            piece = 0.0
            for part, n in spans:
                cols = cols_of(part, n)
                piece = piece + dot(full_x[:, cols], weight[cols, :])
            pre[a] = piece if first else pre[a] + piece

    for n in range(3, early_n - 1):
        land_in(n)
    wait_rows(bo_recv)
    gather_back(back_recv_o)
    for n in range(chunks):
        at = local_cols(n)
        held = back_rows[:, at]
        out_sum[:, at] = dot(factor_high[...], held) + dot(factor_low[...], held)
    for n in range(early_n - 1):
        arrived(n)
    add_in([(source_t(st), n) for n in range(early_n - 1) for st in range(nt)], first=True)
    land_in(early_n - 1)
    finish_grad()
    land_in(early_n)
    add_in([(me_t, early_n - 1)])
    arrived(early_n - 1)
    add_in([(source_t(st), early_n - 1) for st in range(1, nt)])

    pre_copies = [
        remote(
            pre, pre_peer.at[st - 1], send_sem, pre_recv.at[st - 1], {"tensor": peer_t(st)},
        )
        for st in range(1, nt)
    ]
    for copy in down_copies:
        copy.wait_recv()
    received(late_w, late_recv)

    def late_piece(unit, a, part, n):
        cols = cols_of(part, n)
        if unit:
            at = (n - early_n) * cw
            return dot(full_x[:, cols], late_w[a, unit - 1, part, at:at + cw, :])
        return dot(full_x[:, cols], (gate_s, up_s)[a][cols, :])

    xf_copies.append(forwards(full_x, chunks - 1, xf_recv))

    def land_last():
        x_copies[chunks - 1].wait_recv()
        for copy in xf_copies[chunks - 1]:
            copy.start()

    def add_late():
        for n in range(early_n, chunks - 1):
            arrived(n)
        for unit in range(nt):
            for a in range(2):
                total = pre[a] if unit == 0 else 0.0
                for n in range(early_n, chunks - 1):
                    for st in range(nt):
                        total = total + late_piece(unit, a, source_t(st), n)
                late[unit, a] = total

    @pl.when(lax.rem(me_t, 2) == 0)
    def _():
        add_late()
        land_last()

    @pl.when(lax.rem(me_t, 2) != 0)
    def _():
        land_last()
        add_late()

    for unit in range(nt):
        for a in range(2):
            late[unit, a] = late[unit, a] + late_piece(unit, a, me_t, chunks - 1)
    for copy in pre_copies:
        copy.wait_recv()
    arrived(chunks - 1)
    for unit in range(nt):
        total = [late[unit, 0], late[unit, 1]]
        for a in range(2):
            if unit:
                total[a] = total[a] + pre_peer[unit - 1, a]
            for st in range(1, nt):
                total[a] = total[a] + late_piece(unit, a, source_t(st), chunks - 1)
        hidden[unit] = (swish(total[0]) * total[1]).astype(BF16)
    for n in range(chunks):
        at = local_cols(n)
        total = out_sum[:, at] + dot(hidden[0], down_s[:, cols_of(me_t, n)])
        for st in range(1, nt):
            total = total + dot(hidden[st], down_peer[st - 1, :, at])
        out_ref[:, at] = total.astype(BF16)

    planned(drain, drain, send_sem, send_sem, {"pipe": nxt}).wait_send()


def store(out, grad, out_hbm, grad_hbm, sem):
    first = pltpu.make_async_copy(out, out_hbm, sem.at[0])
    second = pltpu.make_async_copy(grad, grad_hbm, sem.at[1])
    first.start()
    second.start()
    first.wait()
    second.wait()


def lanes_last(choices):
    return jnp.swapaxes(choices[:, 0], 1, 2)


def in_hbm(values):
    return pltpu.with_memory_space_constraint(values, pltpu.HBM)


def local(
    inputs_prev, cotangent_next, saved_input, expert_ids, keep_mask, slot_pos, weight_q,
    gate_routed, up_routed, down_routed, gate_shared, up_shared, down_shared,
):
    n_pipe, ne, nt = lax.axis_size("pipe"), lax.axis_size("expert"), lax.axis_size("tensor")
    tokens, width = inputs_prev.shape[1:]
    topk = expert_ids.shape[3]
    features = width * nt
    capacity = tokens // 32
    experts = ne // 2
    blocks = -(-experts * capacity // BLOCK)
    folded = width // 2 if width % 256 == 0 else width
    fr, fs = gate_routed.shape[3], gate_shared.shape[2]
    chunks = width // chunk_of(width)
    peers = ne * nt - 1
    sent_bytes = (
        3 * topk * tokens * 4
        + (2 + 3 * (nt - 1)) * tokens * width * 2
        + (nt - 1) * fs * width * 2
        + 2 * (nt - 1) * nt * LATE * chunk_of(width) * fs * 2
        + 5 * peers * BLOCK * folded * 2
        + blocks * BLOCK * width * 2
        + (nt - 1) * tokens * width * 4
        + (nt - 1) * 2 * tokens * fs * 4
    )
    vmem = pl.BlockSpec(memory_space=pltpu.VMEM)
    hbm = pl.BlockSpec(memory_space=pl.ANY)
    dma = pltpu.SemaphoreType.DMA
    shape = pltpu.VMEM((tokens, width), BF16)
    out, grad = pl.pallas_call(
        functools.partial(kernel, (n_pipe, ne, nt, capacity)),
        out_shape=(shape, shape),
        in_specs=[hbm] * 13,
        out_specs=(vmem, vmem),
        scratch_shapes=[
            pltpu.VMEM((features, fr), BF16),
            pltpu.VMEM((features, fr), BF16),
            pltpu.VMEM((fr, features), BF16),
            pltpu.VMEM((features, fs), BF16),
            pltpu.VMEM((features, fs), BF16),
            pltpu.VMEM((fs, features), BF16),
            pltpu.VMEM((nt - 1, fs, width), BF16),
            pltpu.VMEM((4, 2, topk, tokens), jnp.int32),
            pltpu.VMEM((3, topk, tokens), jnp.int32),
            pltpu.VMEM((tokens, width), BF16),
            pltpu.VMEM((tokens, width), BF16),
            pltpu.VMEM((tokens, features), BF16),
            pltpu.VMEM((tokens, features), BF16),
            pltpu.VMEM((tokens, features), BF16),
            pltpu.VMEM((tokens, fs), F32),
            pltpu.VMEM((tokens, fs), F32),
            pltpu.VMEM((tokens, fs), F32),
            pltpu.VMEM((2, tokens, fs), F32),
            pltpu.VMEM((nt - 1, 2, tokens, fs), F32),
            pltpu.VMEM((nt, 2, tokens, fs), F32),
            pltpu.VMEM((2, nt - 1, nt, LATE * chunk_of(width), fs), BF16),
            pltpu.VMEM((nt, tokens, fs), BF16),
            pltpu.VMEM((sent_bytes // 256, 128), BF16),
            pltpu.VMEM((tokens, fs), BF16),
            pltpu.VMEM((tokens, fs), BF16),
            pltpu.VMEM((ne * capacity, fr), F32),
            pltpu.VMEM((ne * capacity, fr), F32),
            pltpu.VMEM((experts, BLOCK, folded), BF16),
            pltpu.VMEM((experts, BLOCK, folded), BF16),
            pltpu.VMEM((blocks, BLOCK, width), BF16),
            pltpu.VMEM((blocks, BLOCK, width), BF16),
            pltpu.VMEM((experts, BLOCK, folded), BF16),
            pltpu.VMEM((ne, nt, BLOCK, folded), BF16),
            pltpu.VMEM((ne, nt, BLOCK, folded), BF16),
            pltpu.VMEM((ne, nt, BLOCK, folded), BF16),
            pltpu.VMEM((ne * capacity, features), BF16),
            pltpu.VMEM((ne, nt, BLOCK, folded), BF16),
            pltpu.VMEM((ne, nt, BLOCK, folded), BF16),
            pltpu.VMEM((ne, nt, BLOCK, folded), BF16),
            pltpu.VMEM((ne, nt, BLOCK, folded), BF16),
            pltpu.VMEM((ne * nt * capacity, width), BF16),
            pltpu.VMEM((fr, features), BF16),
            pltpu.VMEM((fr, features), BF16),
            pltpu.VMEM((features, fr), BF16),
            pltpu.VMEM((fs, features), BF16),
            pltpu.VMEM((fs, features), BF16),
            pltpu.VMEM((nt, tokens, width), F32),
            pltpu.VMEM((nt - 1, tokens, width), F32),
            pltpu.VMEM((tokens, width), F32),
            pltpu.VMEM((tokens, ne * nt * capacity), BF16),
            pltpu.VMEM((tokens, ne * nt * capacity), BF16),
            pltpu.VMEM((tokens, ne * nt * capacity), BF16),
            dma((6,)), dma, dma((3,)), dma, pltpu.SemaphoreType.REGULAR,
            dma, dma((nt - 1,)), dma((nt - 1,)), dma((chunks,)), dma((chunks,)),
            dma((chunks, nt - 1)), dma((chunks, nt - 1)),
            dma, dma, dma, dma, dma, dma, dma((nt - 1,)), dma((nt - 1,)), dma,
        ],
        compiler_params=pltpu.CompilerParams(
            collective_id=0, has_side_effects=True, vmem_limit_bytes=60 * 1024 * 1024
        ),
        name="moe_step",
    )(
        *(in_hbm(v) for v in (
            inputs_prev[0], cotangent_next[0], saved_input[0],
            *(lanes_last(v) for v in (expert_ids, keep_mask, slot_pos, weight_q)),
            gate_routed[0, 0], up_routed[0, 0], down_routed[0, 0],
            gate_shared[0], up_shared[0], down_shared[0],
        ))
    )
    result = jax.ShapeDtypeStruct((tokens, width), BF16)
    out, grad = pl.pallas_call(
        store,
        out_shape=(result, result),
        in_specs=[vmem] * 2,
        out_specs=(hbm, hbm),
        scratch_shapes=[dma((2,))],
        compiler_params=pltpu.CompilerParams(vmem_limit_bytes=2 * 1024 * 1024),
        name="store_out",
    )(*(pltpu.with_memory_space_constraint(v, pltpu.VMEM) for v in (out, grad)))
    return out[None], grad[None]


def solution(mesh):
    return jax.shard_map(
        local,
        mesh=mesh,
        in_specs=(
            P("pipe", "expert", "tensor"),
            P("pipe", "expert", "tensor"),
            P("pipe", "expert", "tensor"),
            P(None, "pipe", "expert", None),
            P(None, "pipe", "expert", None),
            P(None, "pipe", "expert", None),
            P(None, "pipe", "expert", None),
            P("pipe", "expert", None, "tensor"),
            P("pipe", "expert", None, "tensor"),
            P("pipe", "expert", "tensor", None),
            P("pipe", None, "tensor"),
            P("pipe", None, "tensor"),
            P("pipe", "tensor", None),
        ),
        out_specs=(P("pipe", "expert", "tensor"), P("pipe", "expert", "tensor")),
        check_vma=False,
    )
```

```python
import functools

import jax
import jax.numpy as jnp
from jax import lax
from jax.experimental import pallas as pl
from jax.experimental.pallas import tpu as pltpu
from jax.sharding import PartitionSpec as P

MESH = pl.DeviceIdType.MESH
F32 = jnp.float32
BF16 = jnp.bfloat16
BLOCK = 8
FIRST_COT = 3
EARLY_IN = 1
LATE = 2
RELAY_AT = 5
EARLY_TURNS = 2
INPUT_GATE = 3


def swish(values):
    return values * jax.nn.sigmoid(values)


def swish_slope(values):
    logistic = jax.nn.sigmoid(values)
    return logistic * (1.0 + values * (1.0 - logistic))


def dot(left, right):
    return jnp.dot(left, right, preferred_element_type=F32)


def contract_last(left, right):
    return lax.dot_general(left, right, (((1,), (1,)), ((), ())), preferred_element_type=F32)


def chunk_of(width):
    return 256 if width % 256 == 0 else 128


def kernel(
    sizes,
    x_hbm, c_hbm, saved_hbm, ids_hbm, keep_hbm, slot_hbm, level_hbm,
    gate_r_hbm, up_r_hbm, down_r_hbm, gate_s_hbm, up_s_hbm, down_s_hbm,
    out_ref, grad_ref,
    gate_r, up_r, down_r, gate_s, up_s, down_s, down_peer,
    tables, tables_next, x_own, c_own, full_x, full_c, full_s,
    a_saved, b_saved, grad_hid, pre, pre_peer, late, late_w, hidden, drain, grad_gate, grad_up,
    a_routed, b_routed,
    send_s, send_c, send_x, held_x, relay_x, recv_s, recv_c, recv_x, rows,
    back_send_g, back_recv_g, back_send_o, back_recv_o, back_rows,
    gate_rt, up_rt, down_rt, gate_st, up_st,
    part_grad, peer_grad, out_sum, factor_high, factor_low, factor_grad,
    weight_sem, table_sem, local_sem, send_sem, entry_sem,
    next_recv, saved_recv, down_recv, c_recv, x_recv, cf_recv, xf_recv,
    rs_recv, rc_recv, rx_recv, pick_recv, bg_recv, bo_recv, part_recv, pre_recv, late_recv,
):
    n_pipe, ne, nt, capacity = sizes
    tokens, width = x_own.shape
    features = width * nt
    experts, blocks = send_s.shape[0], send_x.shape[0]
    folds = width // send_s.shape[2]
    peers = ne * nt - 1
    row_lines = BLOCK * send_s.shape[2] // 128
    me_p, me_e, me_t = lax.axis_index("pipe"), lax.axis_index("expert"), lax.axis_index("tensor")
    nxt, prv = lax.rem(me_p + 1, n_pipe), lax.rem(me_p + n_pipe - 1, n_pipe)
    my_cols = pl.ds(pl.multiple_of(me_t * width, 128), width)
    cw = chunk_of(width)
    chunks = width // cw
    last_p = n_pipe - 1

    def peer_t(step):
        return lax.rem(me_t + step, nt)

    def peer_e(step):
        return lax.rem(me_e + step, ne)

    def source_t(step):
        return lax.rem(me_t + nt - step, nt)

    def planned(src, dst, ssem, rsem, device):
        return pltpu.make_async_remote_copy(
            src_ref=src, dst_ref=dst, send_sem=ssem, recv_sem=rsem,
            device_id=device, device_id_type=MESH,
        )

    def remote(src, dst, ssem, rsem, device):
        copy = planned(src, dst, ssem, rsem, device)
        copy.start()
        return copy

    def received(whole, sem):
        planned(whole, whole, sem, sem, {"pipe": nxt}).wait_recv()

    def load(src, dst, sem):
        copy = pltpu.make_async_copy(src, dst, sem)
        copy.start()
        return copy

    def local_cols(n):
        return pl.ds(n * cw, cw)

    def cols_of(part, n):
        return pl.ds(pl.multiple_of(part * width + n * cw, 128), cw)

    c_load = load(c_hbm, c_own, local_sem.at[0])
    for a, src in enumerate((ids_hbm, keep_hbm, slot_hbm, level_hbm)):
        load(src, tables.at[a], table_sem)
    saved_load = load(saved_hbm, full_s.at[:, my_cols], local_sem.at[1])
    x_load = load(x_hbm, x_own, local_sem.at[2])

    barrier = pltpu.get_barrier_semaphore()
    mate = me_e + 1 - 2 * lax.rem(me_e, 2)
    greeted = [{"pipe": nxt}, {"pipe": prv}]
    for st in range(nt):
        greeted.append({"expert": mate, "tensor": peer_t(st)})
        for se in range(0, ne, 2):
            if se or st:
                greeted.append({"expert": peer_e(se), "tensor": peer_t(st)})
    for device in greeted:
        pl.semaphore_signal(barrier, inc=1, device_id=device, device_id_type=MESH)
    c_load.wait()
    gate_s_load = load(gate_s_hbm, gate_s, weight_sem.at[0])
    up_s_load = load(up_s_hbm, up_s, weight_sem.at[1])
    gate_r_load = load(gate_r_hbm, gate_r, weight_sem.at[2])
    up_r_load = load(up_r_hbm, up_r, weight_sem.at[3])
    down_s_load = load(down_s_hbm, down_s, weight_sem.at[4])
    down_r_load = load(down_r_hbm, down_r, weight_sem.at[5])
    pl.semaphore_wait(barrier, len(greeted))
    pl.semaphore_signal(entry_sem, inc=1, device_id={"expert": mate}, device_id_type=MESH)

    pltpu.make_async_copy(tables, tables, table_sem).wait()
    for a in range(3):
        remote(tables.at[a, 0], tables_next.at[a], send_sem, next_recv, {"pipe": prv})
    c_copies = [
        planned(
            c_own.at[:, local_cols(n)], full_c.at[:, cols_of(me_t, n)],
            send_sem, c_recv.at[n], {"pipe": prv},
        )
        for n in range(chunks)
    ]
    x_copies = [
        planned(
            x_own.at[:, local_cols(n)], full_x.at[:, cols_of(me_t, n)],
            send_sem, x_recv.at[n], {"pipe": nxt},
        )
        for n in range(chunks)
    ]
    for n in range(FIRST_COT):
        c_copies[n].start()
    saved_load.wait()
    x_load.wait()
    saved_copies = [
        remote(
            full_s.at[:, my_cols], full_s.at[:, my_cols], send_sem,
            saved_recv.at[st - 1], {"tensor": peer_t(st)},
        )
        for st in range(1, nt)
    ]
    down_copies = []
    for st in range(1, nt):
        to = peer_t(st)
        down_copies.append(remote(
            down_s_hbm.at[:, pl.ds(pl.multiple_of(to * width, 128), width)], down_peer.at[st - 1],
            send_sem, down_recv.at[st - 1], {"tensor": to},
        ))
        for part in range(nt):
            at = pl.ds(part * width + (chunks - LATE) * cw, LATE * cw)
            for a, src in enumerate((gate_s_hbm, up_s_hbm)):
                remote(
                    src.at[at, :], late_w.at[a, st - 1, part], send_sem, late_recv, {"tensor": to}
                )

    def table(target, values, slots_at):
        total = jnp.zeros((slots_at.shape[0], tokens), jnp.int32)
        for k in range(target.shape[0]):
            total = total + jnp.where(target[k:k + 1] == slots_at, values[k:k + 1], 0)
        return total

    def targets(ids, keep, slot):
        return jnp.where(keep > 0, ids * capacity + slot, -1)

    target_f = targets(tables[0, 0], tables[1, 0], tables[2, 0])
    target_b = targets(tables[0, 1], tables[1, 1], tables[2, 1])
    level_f, level_b = tables[3, 0], tables[3, 1]
    used = max(16, blocks * BLOCK)
    place = lax.broadcasted_iota(jnp.int32, (used, tokens), 0)
    ones = jnp.ones(target_f.shape, jnp.int32)
    pick_b = table(target_b, ones, place).astype(F32).astype(BF16)
    scale_b = jnp.sum(table(target_b, level_b, place).astype(F32), axis=1, keepdims=True) / 4096.0

    def pack(values):
        half = width // folds
        return jnp.concatenate((values[:, :half], values[:, width - half:]), axis=0).astype(BF16)

    def unpack(values):
        held = values.astype(F32)
        pieces = [held[f * capacity:(f + 1) * capacity] for f in range(folds)]
        return jnp.concatenate(pieces, axis=1)

    def exchange(buffer, landing, rsem):
        for se in range(ne):
            for st in range(nt):
                if se or st:
                    to_e = peer_e(se)
                    remote(
                        buffer.at[lax.div(to_e, 2)], landing.at[me_e, me_t], send_sem, rsem,
                        {"expert": to_e, "tensor": peer_t(st)},
                    )
        landing[me_e, me_t] = buffer[lax.div(me_e, 2)]

    def wait_rows(rsem):
        received(drain.at[pl.ds(0, peers * row_lines)], rsem)

    group = 16 // capacity

    def gather_rows(landing):
        for t in range(nt):
            for i in range(0, ne, group):
                held = [unpack(landing[j, t]) for j in range(i, i + group)]
                rows[i * capacity:(i + group) * capacity, t * width:(t + 1) * width] = (
                    jnp.concatenate(held, axis=0).astype(BF16)
                )

    def pick_rows(picks, read):
        return jnp.concatenate([dot(picks, read(n)) for n in range(chunks)], axis=1)

    def fill(buffer, picked):
        for k in range(experts):
            buffer[k] = pack(picked[k * capacity:(k + 1) * capacity])

    fill(send_s, pick_rows(pick_b, lambda n: full_s[:, cols_of(me_t, n)]))
    pl.semaphore_wait(entry_sem, 1)
    exchange(send_s, recv_s, rs_recv)

    parts = ne * nt * capacity
    place_b = lax.broadcasted_iota(jnp.int32, (parts, tokens), 0)
    expert = lax.div(lax.div(place_b, nt * capacity), 2)
    slots = expert * capacity + lax.rem(place_b, capacity)
    level = table(target_f, level_f, slots)
    high = lax.div(level, 64)
    low = level - high * 64
    factor_high[...] = (high.astype(F32) / 64.0).T.astype(BF16)
    factor_low[...] = (low.astype(F32) / 4096.0).T.astype(BF16)
    factor_grad[...] = table(target_b, ones, slots).astype(F32).T.astype(BF16)

    for copy in saved_copies:
        copy.wait_recv()
    gate_s_load.wait()
    up_s_load.wait()
    cs = chunk_of(gate_s.shape[1])

    for n in range(gate_s.shape[1] // cs):
        cols = pl.ds(n * cs, cs)
        gate_back = dot(full_s[...], gate_s[:, cols])
        up_back = dot(full_s[...], up_s[:, cols])
        a_saved[:, cols] = up_back * swish_slope(gate_back)
        b_saved[:, cols] = swish(gate_back)

    received(tables_next, next_recv)
    target_n = targets(tables_next[0], tables_next[1], tables_next[2])
    pick_n = table(target_n, ones, place).astype(F32).astype(BF16)

    picked = pick_rows(pick_n, lambda n: x_own[:, local_cols(n)])
    for b in range(blocks):
        send_x[b] = picked[b * BLOCK:(b + 1) * BLOCK].astype(BF16)
    picked_copy = remote(send_x, held_x, send_sem, pick_recv, {"pipe": nxt})

    order = [(c_copies, n) for n in range(FIRST_COT, chunks)]
    early = list(order)
    for m in range(EARLY_IN):
        early.insert(len(early) - 2 * EARLY_IN + 1 + 2 * m, (x_copies, m))

    @pl.when(me_p == last_p)
    def _():
        for kind, n in early:
            kind[n].start()

    @pl.when(me_p != last_p)
    def _():
        for kind, n in order:
            kind[n].start()

    for load_done in (gate_r_load, up_r_load, down_r_load):
        load_done.wait()
    turned = features // chunks

    def turn(n):
        at = pl.ds(n * turned, turned)
        gate_st[:, at] = gate_s[at, :].T
        up_st[:, at] = up_s[at, :].T
        gate_rt[:, at] = gate_r[at, :].T
        up_rt[:, at] = up_r[at, :].T
        down_rt[at, :] = down_r[:, at].T

    for n in range(EARLY_TURNS):
        turn(n)

    wait_rows(rs_recv)
    gather_rows(recv_s)
    gate_back = dot(rows[...], gate_r[...])
    a_routed[...] = dot(rows[...], up_r[...]) * swish_slope(gate_back)
    b_routed[...] = swish(gate_back)

    down_s_load.wait()

    def forwards(held, n, rsem):
        cols = cols_of(me_t, n)
        return [
            planned(
                held.at[:, cols], held.at[:, cols], send_sem, rsem(n).at[st - 1],
                {"tensor": peer_t(st)},
            )
            for st in range(1, nt)
        ]

    def forward(held, n, rsem):
        copies = forwards(held, n, rsem)
        for copy in copies:
            copy.start()
        return copies

    def add_cot(part, n, first=False):
        cols = cols_of(part, n)
        piece = contract_last(full_c[:, cols], down_s[:, cols])
        grad_hid[...] = piece if first else grad_hid[...] + piece

    def add_forwarded(copies, n, add):
        for st in range(1, nt):
            copies[st - 1].wait_recv()
            add(source_t(st), n)

    cf_copies = []
    for n in range(chunks):
        c_copies[n].wait_recv()
        cf_copies.append(forward(full_c, n, lambda m: cf_recv.at[m]))
        if n == INPUT_GATE:
            @pl.when(me_p != last_p)
            def _():
                for m in range(EARLY_IN):
                    x_copies[m].start()

            for m in range(EARLY_IN, chunks):
                x_copies[m].start()
        if n == chunks - 1:
            fill(send_c, scale_b * pick_rows(pick_b, lambda m: full_c[:, cols_of(me_t, m)]))
            exchange(send_c, recv_c, rc_recv)
        if n == RELAY_AT:
            picked_copy.wait_recv()
            for k in range(experts):
                b, at = divmod(k * capacity, BLOCK)
                relay_x[k] = pack(held_x[b].astype(F32)[at:at + capacity])
            exchange(relay_x, recv_x, rx_recv)
        add_cot(me_t, n, first=n == 0)
        if n + EARLY_TURNS < chunks:
            turn(n + EARLY_TURNS)
        if n:
            add_forwarded(cf_copies[n - 1], n - 1, add_cot)
    xf_copies = []

    def input_sem(n):
        return xf_recv.at[max(n - (chunks - LATE - 2), 0)]

    def land_in(n):
        x_copies[n].wait_recv()
        xf_copies.append(forward(full_x, n, input_sem))

    def send_back(total_of, buffer, landing, rsem):
        for st in list(range(1, nt)) + [0]:
            to_t = peer_t(st)
            total = jnp.concatenate([total_of(cols_of(to_t, n)) for n in range(chunks)], axis=1)
            for i in range(ne):
                buffer[i, to_t] = pack(total[i * capacity:(i + 1) * capacity])
            for se in range(ne):
                if se or st:
                    to_e = peer_e(se)
                    remote(
                        buffer.at[to_e, to_t], landing.at[me_e, me_t], send_sem, rsem,
                        {"expert": to_e, "tensor": to_t},
                    )
        landing[me_e, me_t] = buffer[me_e, me_t]

    add_forwarded(cf_copies[chunks - 1], chunks - 1, add_cot)
    grad_gate[...] = (grad_hid[...] * a_saved[...]).astype(BF16)
    grad_up[...] = (grad_hid[...] * b_saved[...]).astype(BF16)
    part_copies = []
    for st in list(range(1, nt)) + [0]:
        to = peer_t(st)
        for n in range(chunks):
            cols = cols_of(to, n)
            part_grad[st, :, local_cols(n)] = (
                dot(grad_gate[...], gate_st[:, cols]) + dot(grad_up[...], up_st[:, cols])
            )
        if st:
            part_copies.append(remote(
                part_grad.at[st], peer_grad.at[st - 1], send_sem,
                part_recv.at[st - 1], {"tensor": to},
            ))
    land_in(0)

    wait_rows(rx_recv)
    gather_rows(recv_x)
    gate_fwd = dot(rows[...], gate_r[...])
    hidden_r = (swish(gate_fwd) * dot(rows[...], up_r[...])).astype(BF16)
    send_back(
        lambda cols: dot(hidden_r, down_r[:, cols]), back_send_o, back_recv_o, bo_recv
    )
    wait_rows(rc_recv)
    gather_rows(recv_c)
    grad_back = dot(rows[...], down_rt[...])
    gate_grad_r = (grad_back * a_routed[...]).astype(BF16)
    up_grad_r = (grad_back * b_routed[...]).astype(BF16)
    send_back(
        lambda cols: dot(gate_grad_r, gate_rt[:, cols]) + dot(up_grad_r, up_rt[:, cols]),
        back_send_g, back_recv_g, bg_recv,
    )
    land_in(1)

    land_in(2)

    def gather_back(landing):
        for i in range(0, ne * nt, group):
            held = [unpack(landing[divmod(j, nt)]) for j in range(i, i + group)]
            back_rows[i * capacity:(i + group) * capacity, :] = (
                jnp.concatenate(held, axis=0).astype(BF16)
            )

    def finish_grad():
        wait_rows(bg_recv)
        gather_back(back_recv_g)
        for copy in part_copies:
            copy.wait_recv()

        for n in range(chunks):
            at = local_cols(n)
            total = part_grad[0, :, at] + dot(factor_grad[...], back_rows[:, at])
            for st in range(1, nt):
                total = total + peer_grad[st - 1, :, at]
            grad_ref[:, at] = total.astype(BF16)

    early_n = chunks - LATE

    def arrived(n):
        for copy in xf_copies[n]:
            copy.wait_recv()

    def add_in(spans, first=False):
        for a, weight in enumerate((gate_s, up_s)):
            piece = 0.0
            for part, n in spans:
                cols = cols_of(part, n)
                piece = piece + dot(full_x[:, cols], weight[cols, :])
            pre[a] = piece if first else pre[a] + piece

    for n in range(3, early_n - 1):
        land_in(n)
    wait_rows(bo_recv)
    gather_back(back_recv_o)
    for n in range(chunks):
        at = local_cols(n)
        held = back_rows[:, at]
        out_sum[:, at] = dot(factor_high[...], held) + dot(factor_low[...], held)
    for st in range(1, nt):
        received(full_x.at[:, pl.ds(0, (early_n - 1) * cw)], xf_recv.at[0, st - 1])
    add_in([(source_t(st), n) for n in range(early_n - 1) for st in range(nt)], first=True)
    land_in(early_n - 1)
    finish_grad()
    land_in(early_n)
    add_in([(me_t, early_n - 1)])
    arrived(early_n - 1)
    add_in([(source_t(st), early_n - 1) for st in range(1, nt)])

    pre_copies = [
        remote(
            pre, pre_peer.at[st - 1], send_sem, pre_recv.at[st - 1], {"tensor": peer_t(st)},
        )
        for st in range(1, nt)
    ]
    for copy in down_copies:
        copy.wait_recv()
    received(late_w, late_recv)

    def late_piece(unit, a, part, n):
        cols = cols_of(part, n)
        if unit:
            at = (n - early_n) * cw
            return dot(full_x[:, cols], late_w[a, unit - 1, part, at:at + cw, :])
        return dot(full_x[:, cols], (gate_s, up_s)[a][cols, :])

    xf_copies.append(forwards(full_x, chunks - 1, input_sem))

    def land_last():
        x_copies[chunks - 1].wait_recv()
        for copy in xf_copies[chunks - 1]:
            copy.start()

    def add_late():
        for n in range(early_n, chunks - 1):
            arrived(n)
        for unit in range(nt):
            for a in range(2):
                total = pre[a] if unit == 0 else 0.0
                for n in range(early_n, chunks - 1):
                    for st in range(nt):
                        total = total + late_piece(unit, a, source_t(st), n)
                late[unit, a] = total

    @pl.when(lax.rem(me_t, 2) == 0)
    def _():
        add_late()
        land_last()

    @pl.when(lax.rem(me_t, 2) != 0)
    def _():
        land_last()
        add_late()

    for unit in range(nt):
        for a in range(2):
            late[unit, a] = late[unit, a] + late_piece(unit, a, me_t, chunks - 1)
    for copy in pre_copies:
        copy.wait_recv()
    arrived(chunks - 1)
    for unit in range(nt):
        total = [late[unit, 0], late[unit, 1]]
        for a in range(2):
            if unit:
                total[a] = total[a] + pre_peer[unit - 1, a]
            for st in range(1, nt):
                total[a] = total[a] + late_piece(unit, a, source_t(st), chunks - 1)
        hidden[unit] = (swish(total[0]) * total[1]).astype(BF16)
    for n in range(chunks):
        at = local_cols(n)
        total = out_sum[:, at] + dot(hidden[0], down_s[:, cols_of(me_t, n)])
        for st in range(1, nt):
            total = total + dot(hidden[st], down_peer[st - 1, :, at])
        out_ref[:, at] = total.astype(BF16)

    planned(drain, drain, send_sem, send_sem, {"pipe": nxt}).wait_send()


def store(out, grad, out_hbm, grad_hbm, sem):
    first = pltpu.make_async_copy(out, out_hbm, sem.at[0])
    second = pltpu.make_async_copy(grad, grad_hbm, sem.at[1])
    first.start()
    second.start()
    first.wait()
    second.wait()


def lanes_last(choices):
    return jnp.swapaxes(choices[:, 0], 1, 2)


def in_hbm(values):
    return pltpu.with_memory_space_constraint(values, pltpu.HBM)


def local(
    inputs_prev, cotangent_next, saved_input, expert_ids, keep_mask, slot_pos, weight_q,
    gate_routed, up_routed, down_routed, gate_shared, up_shared, down_shared,
):
    n_pipe, ne, nt = lax.axis_size("pipe"), lax.axis_size("expert"), lax.axis_size("tensor")
    tokens, width = inputs_prev.shape[1:]
    topk = expert_ids.shape[3]
    features = width * nt
    capacity = tokens // 32
    experts = ne // 2
    blocks = -(-experts * capacity // BLOCK)
    folded = width // 2 if width % 256 == 0 else width
    fr, fs = gate_routed.shape[3], gate_shared.shape[2]
    chunks = width // chunk_of(width)
    peers = ne * nt - 1
    sent_bytes = (
        3 * topk * tokens * 4
        + (2 + 3 * (nt - 1)) * tokens * width * 2
        + (nt - 1) * fs * width * 2
        + 2 * (nt - 1) * nt * LATE * chunk_of(width) * fs * 2
        + 5 * peers * BLOCK * folded * 2
        + blocks * BLOCK * width * 2
        + (nt - 1) * tokens * width * 4
        + (nt - 1) * 2 * tokens * fs * 4
    )
    vmem = pl.BlockSpec(memory_space=pltpu.VMEM)
    hbm = pl.BlockSpec(memory_space=pl.ANY)
    dma = pltpu.SemaphoreType.DMA
    shape = pltpu.VMEM((tokens, width), BF16)
    out, grad = pl.pallas_call(
        functools.partial(kernel, (n_pipe, ne, nt, capacity)),
        out_shape=(shape, shape),
        in_specs=[hbm] * 13,
        out_specs=(vmem, vmem),
        scratch_shapes=[
            pltpu.VMEM((features, fr), BF16),
            pltpu.VMEM((features, fr), BF16),
            pltpu.VMEM((fr, features), BF16),
            pltpu.VMEM((features, fs), BF16),
            pltpu.VMEM((features, fs), BF16),
            pltpu.VMEM((fs, features), BF16),
            pltpu.VMEM((nt - 1, fs, width), BF16),
            pltpu.VMEM((4, 2, topk, tokens), jnp.int32),
            pltpu.VMEM((3, topk, tokens), jnp.int32),
            pltpu.VMEM((tokens, width), BF16),
            pltpu.VMEM((tokens, width), BF16),
            pltpu.VMEM((tokens, features), BF16),
            pltpu.VMEM((tokens, features), BF16),
            pltpu.VMEM((tokens, features), BF16),
            pltpu.VMEM((tokens, fs), F32),
            pltpu.VMEM((tokens, fs), F32),
            pltpu.VMEM((tokens, fs), F32),
            pltpu.VMEM((2, tokens, fs), F32),
            pltpu.VMEM((nt - 1, 2, tokens, fs), F32),
            pltpu.VMEM((nt, 2, tokens, fs), F32),
            pltpu.VMEM((2, nt - 1, nt, LATE * chunk_of(width), fs), BF16),
            pltpu.VMEM((nt, tokens, fs), BF16),
            pltpu.VMEM((sent_bytes // 256, 128), BF16),
            pltpu.VMEM((tokens, fs), BF16),
            pltpu.VMEM((tokens, fs), BF16),
            pltpu.VMEM((ne * capacity, fr), F32),
            pltpu.VMEM((ne * capacity, fr), F32),
            pltpu.VMEM((experts, BLOCK, folded), BF16),
            pltpu.VMEM((experts, BLOCK, folded), BF16),
            pltpu.VMEM((blocks, BLOCK, width), BF16),
            pltpu.VMEM((blocks, BLOCK, width), BF16),
            pltpu.VMEM((experts, BLOCK, folded), BF16),
            pltpu.VMEM((ne, nt, BLOCK, folded), BF16),
            pltpu.VMEM((ne, nt, BLOCK, folded), BF16),
            pltpu.VMEM((ne, nt, BLOCK, folded), BF16),
            pltpu.VMEM((ne * capacity, features), BF16),
            pltpu.VMEM((ne, nt, BLOCK, folded), BF16),
            pltpu.VMEM((ne, nt, BLOCK, folded), BF16),
            pltpu.VMEM((ne, nt, BLOCK, folded), BF16),
            pltpu.VMEM((ne, nt, BLOCK, folded), BF16),
            pltpu.VMEM((ne * nt * capacity, width), BF16),
            pltpu.VMEM((fr, features), BF16),
            pltpu.VMEM((fr, features), BF16),
            pltpu.VMEM((features, fr), BF16),
            pltpu.VMEM((fs, features), BF16),
            pltpu.VMEM((fs, features), BF16),
            pltpu.VMEM((nt, tokens, width), F32),
            pltpu.VMEM((nt - 1, tokens, width), F32),
            pltpu.VMEM((tokens, width), F32),
            pltpu.VMEM((tokens, ne * nt * capacity), BF16),
            pltpu.VMEM((tokens, ne * nt * capacity), BF16),
            pltpu.VMEM((tokens, ne * nt * capacity), BF16),
            dma((6,)), dma, dma((3,)), dma, pltpu.SemaphoreType.REGULAR,
            dma, dma((nt - 1,)), dma((nt - 1,)), dma((chunks,)), dma((chunks,)),
            dma((chunks, nt - 1)), dma((LATE + 2, nt - 1)),
            dma, dma, dma, dma, dma, dma, dma((nt - 1,)), dma((nt - 1,)), dma,
        ],
        compiler_params=pltpu.CompilerParams(
            collective_id=0, has_side_effects=True, vmem_limit_bytes=60 * 1024 * 1024
        ),
        name="moe_step",
    )(
        *(in_hbm(v) for v in (
            inputs_prev[0], cotangent_next[0], saved_input[0],
            *(lanes_last(v) for v in (expert_ids, keep_mask, slot_pos, weight_q)),
            gate_routed[0, 0], up_routed[0, 0], down_routed[0, 0],
            gate_shared[0], up_shared[0], down_shared[0],
        ))
    )
    result = jax.ShapeDtypeStruct((tokens, width), BF16)
    out, grad = pl.pallas_call(
        store,
        out_shape=(result, result),
        in_specs=[vmem] * 2,
        out_specs=(hbm, hbm),
        scratch_shapes=[dma((2,))],
        compiler_params=pltpu.CompilerParams(vmem_limit_bytes=2 * 1024 * 1024),
        name="store_out",
    )(*(pltpu.with_memory_space_constraint(v, pltpu.VMEM) for v in (out, grad)))
    return out[None], grad[None]


def solution(mesh):
    return jax.shard_map(
        local,
        mesh=mesh,
        in_specs=(
            P("pipe", "expert", "tensor"),
            P("pipe", "expert", "tensor"),
            P("pipe", "expert", "tensor"),
            P(None, "pipe", "expert", None),
            P(None, "pipe", "expert", None),
            P(None, "pipe", "expert", None),
            P(None, "pipe", "expert", None),
            P("pipe", "expert", None, "tensor"),
            P("pipe", "expert", None, "tensor"),
            P("pipe", "expert", "tensor", None),
            P("pipe", None, "tensor"),
            P("pipe", None, "tensor"),
            P("pipe", "tensor", None),
        ),
        out_specs=(P("pipe", "expert", "tensor"), P("pipe", "expert", "tensor")),
        check_vma=False,
    )
```
